256 devices in a mesh: mem: 32 (over z, x), tp: 8 (over y, core).
Axes of the slice: x: 4, y: 4, z: 8, core: 2. Of those that a mesh axis runs over, the one named last changes fastest.
Arguments:
- tokens: bfloat16 [16384, 5120], P('mem'), may hold values from -6 to 6
- query_weight: bfloat16 [5120, 5120], P('mem', 'tp'), may hold values from -0.078125 to 0.078125
- output_weight: bfloat16 [5120, 5120], P('tp', 'mem'), may hold values from -0.078125 to 0.078125
- time_modulation: float32 [50, 2, 5120], replicated, may hold values from -3 to 3
- timestep: int32 [1], replicated, may hold values from 0 to 49
- memory_store: bfloat16 [2048, 2, 8, 5120], P('mem', None, None, 'tp'), may hold values from -480 to 480
- retrieved: int32 [16, 8], replicated, may hold values from 0 to 2047, as said below
- fresh_entry: bfloat16 [2, 8, 5120], P(None, None, ('tp', 'mem')), may hold values from -4 to 4
- write_slot: int32 [1], replicated, may hold values from 0 to 2047
Outputs:
- memory_out: bfloat16 [16384, 5120], P('mem', 'tp')
- updated_store: bfloat16 [2048, 2, 8, 5120], P('mem', None, None, 'tp')
The draws below stay inside these ranges and needn't reach their ends.
Inputs may be any that keep to these rules, and one draw needn't show every extreme that they name: `retrieved`: in each row, no two indices lie in the same aligned block of 64 stored frames.
All inputs are finite; a program needn't handle non-finite values.
Results may differ from the reference program's by a relative error of at most 0.014.
The reference program's roundings to bfloat16 on the way count: a program that leaves them out, or rounds other values in their place, can miss the bound.
Values may be sent and summed in bfloat16 or wider, within the bound.
No kernel may reach another device: no remote copies, remote signals or barrier semaphores. Data moves between devices by JAX's collectives and lax.ppermute only.
A program may use at most 128 MiB of HBM per device.

```python
import jax
import jax.numpy as jnp
from jax import lax

D = 5120
HEAD_SIZE = 128
FR_DEV = 64
MT = 8
R = 8
STEPS = 50
TOKENS = 16384
CUR_FRAMES = 16
MEM_FRAMES = 2048
N_TP = 8


def draw_memory_store(key, part):
    first = jax.random.fold_in(key, 0)
    base = jnp.clip(jax.random.normal(first, (MEM_FRAMES, 2, MT, D), jnp.float32), -4.0, 4.0)
    return base.astype(jnp.bfloat16)


def draw_retrieved(key, part):
    first, second, third = jax.random.split(key, 3)
    blocks_all = MEM_FRAMES // FR_DEV
    heat = jax.random.randint(first, (blocks_all,), 0, 4)
    noise = jax.random.randint(second, (CUR_FRAMES, blocks_all), 0, 1024)
    score = (noise + heat[None, :] * 600) * blocks_all + jnp.arange(blocks_all, dtype=jnp.int32)[None, :]
    best, blocks = lax.top_k(score, R)
    offset = jax.random.randint(third, (CUR_FRAMES, R), 0, FR_DEV)
    return (blocks.astype(jnp.int32) * FR_DEV + offset).astype(jnp.int32)


def steps_of(rng, dims, cuts, smallest, largest):
    loudness, own = 1.0, jax.random.fold_in(rng, 6)
    for position, shards_of in cuts:
        heights = jnp.exp(jax.random.uniform(jax.random.fold_in(own, position), (shards_of,), jnp.float32, smallest / len(cuts), largest / len(cuts)))
        loudness = loudness * jnp.repeat(heights, dims[position] // shards_of).reshape([-1 if axis == position else 1 for axis in range(len(dims))])
    return loudness


def scatter_about(key, dims, deviation, bound, shards=(), kind=jnp.bfloat16):
    result = deviation * jax.random.normal(key, dims, jnp.float32)
    if shards:
        result = result * steps_of(key, dims, shards, -0.22, 0.18)
    return jnp.clip(result, -bound, bound).astype(kind)


def setup_inputs(seed: int = 0) -> dict:
    key_list = jax.random.split(jax.random.key(seed), 10)
    tokens = scatter_about(key_list[0], (TOKENS, D), 1.0, 6.0, ((0, 32),))
    query_weight = scatter_about(key_list[1], (D, D), D ** -0.5, 0.078125, ((0, 32), (1, 8)))
    output_weight = scatter_about(key_list[2], (D, D), D ** -0.5, 0.078125, ((0, 8), (1, 32)))
    time_modulation = scatter_about(key_list[3], (STEPS, 2, D), 0.5, 3.0, (), jnp.float32)
    timestep = jax.random.randint(key_list[4], (1,), 0, STEPS).astype(jnp.int32)
    memory_store = draw_memory_store(jax.random.fold_in(key_list[9], 71), 0)
    retrieved = draw_retrieved(jax.random.fold_in(key_list[9], 71), 0)
    fresh_entry = scatter_about(key_list[7], (2, MT, D), 1.0, 4.0, ((2, 256),))
    write_slot = jax.random.randint(key_list[8], (1,), 0, MEM_FRAMES).astype(jnp.int32)
    return {"tokens": tokens, "query_weight": query_weight, "output_weight": output_weight, "time_modulation": time_modulation, "timestep": timestep, "memory_store": memory_store, "retrieved": retrieved, "fresh_entry": fresh_entry, "write_slot": write_slot}


EPS = 1e-06

def attend(query, keys, vals):
    count = query.shape[0]
    query_heads = query.astype(jnp.float32).reshape(count, -1, HEAD_SIZE)
    heads = query_heads.shape[1]
    key_heads = keys.astype(jnp.float32).reshape(-1, heads, HEAD_SIZE)
    value_heads = vals.astype(jnp.float32).reshape(-1, heads, HEAD_SIZE)
    logit_matrix = jnp.einsum('qaz,saz->aqs', query_heads, key_heads) * HEAD_SIZE ** (-0.5)
    top = lax.optimization_barrier(jnp.max(logit_matrix, axis=-1, keepdims=True))
    expo = jnp.exp(logit_matrix - top)
    attention_probs = (expo / lax.optimization_barrier(jnp.sum(expo, axis=-1, keepdims=True))).astype(jnp.bfloat16)
    blended_values = jnp.einsum('gfy,ygp->fgp', attention_probs.astype(jnp.float32), value_heads)
    return blended_values.reshape(count, heads * HEAD_SIZE).astype(jnp.bfloat16)

def reference(tokens, query_weight, output_weight, time_modulation, timestep, memory_store, retrieved, fresh_entry, write_slot):
    modrow = lax.dynamic_index_in_dim(time_modulation, timestep[0], 0, keepdims=False)
    values = tokens.astype(jnp.float32)
    factor = lax.rsqrt(lax.optimization_barrier(jnp.mean(values * values, axis=1, keepdims=True)) + EPS)
    modulated = (values * factor * (1.0 + modrow[0]) + modrow[1]).astype(jnp.bfloat16)
    query = jnp.dot(modulated, query_weight, preferred_element_type=jnp.float32).astype(jnp.bfloat16)
    frames = retrieved.shape[0]
    grouped = query.reshape(frames, -1, D)

    def one_frame(item):
        block, picks = item
        fetched = jnp.take(memory_store, picks, axis=0)
        keys = fetched[:, 0].reshape(R * MT, D)
        vals = fetched[:, 1].reshape(R * MT, D)
        return attend(block, keys, vals)
    attended = lax.map(one_frame, (grouped, retrieved)).reshape(-1, D)
    width = D // N_TP
    total = jnp.zeros((attended.shape[0], D), jnp.float32)
    for group in range(N_TP):
        term = jnp.dot(attended[:, group * width:(group + 1) * width], output_weight[group * width:(group + 1) * width], preferred_element_type=jnp.float32).astype(jnp.bfloat16)
        term = lax.optimization_barrier(term)
        total = total + term.astype(jnp.float32)
    memory_out = total.astype(jnp.bfloat16)
    slots = jnp.arange(memory_store.shape[0], dtype=jnp.int32)
    updated_store = jnp.where((slots == write_slot[0])[:, None, None, None], fresh_entry[None], memory_store)
    return (memory_out, updated_store)
```

```python
import functools

import jax
import jax.numpy as jnp
from jax import lax
from jax.experimental import pallas as pl
from jax.experimental.pallas import tpu as pltpu
from jax.sharding import Mesh
from jax.sharding import PartitionSpec as P

HEAD_SIZE = 128
MEM = ("mem_0", "mem_1")
TP_MEM = ("tp", "mem_0", "mem_1")

EPS = 1e-06


def shift(array, axis, by):
    n = lax.axis_size(axis)
    return lax.ppermute(array, axis, [(i, (i + by) % n) for i in range(n)])


def around(block, axis, whole, direction=1):
    n = lax.axis_size(axis)
    got = [(block, 0, None)]
    fore = back = block
    for step in range(1, (n - 1) // 2 + 1):
        fore, back = shift(fore, axis, 1), shift(back, axis, -1)
        got += [(fore, -step, None), (back, step, None)]
    half = n // 2
    if whole:
        last = shift(fore, axis, 1) if direction > 0 else shift(back, axis, -1)
        got.append((last, half, None))
    else:
        cut = block.shape[0] // 2
        got.append((shift(fore[:cut], axis, 1), half, (0, cut)))
        got.append((shift(back[cut:], axis, -1), half, (cut, block.shape[0])))
    return got


def in_order(got, n):
    return jnp.stack([next(a for a, off, _ in got if off % n == i) for i in range(n)])


def attend_kernel(plan, rows, nz, nx, xm_ref, k_ref, v_ref, *rest):
    pieces, (out_ref, w_ref, acc_ref, sems) = rest[: len(plan)], rest[len(plan):]
    z, x = lax.axis_index("mem_0"), lax.axis_index("mem_1")
    copies = []
    for piece, entries in zip(pieces, plan):
        for index, off_z, off_x, lane, lanes in entries:
            block = lax.rem(z + (off_z % nz), nz) * nx + lax.rem(x + (off_x % nx), nx)
            start = pl.multiple_of(block * rows, 32)
            copy = pltpu.make_async_copy(
                piece.at[index],
                w_ref.at[pl.ds(start, rows), pl.ds(lane, lanes)],
                sems.at[len(copies)],
            )
            copy.start()
            copies.append(copy)
    for copy in copies:
        copy.wait()
    depth = w_ref.shape[0]
    step = depth // 4

    def accumulate(i, carry):
        at = pl.ds(pl.multiple_of(i * step, 128), step)
        acc_ref[...] += jnp.dot(xm_ref[:, at], w_ref[at, :], preferred_element_type=jnp.float32)
        return carry

    acc_ref[...] = jnp.zeros_like(acc_ref)
    lax.fori_loop(0, 4, accumulate, 0)
    for head in range(w_ref.shape[1] // HEAD_SIZE):
        at = pl.ds(head * HEAD_SIZE, HEAD_SIZE)
        query = acc_ref[:, at].astype(jnp.bfloat16)
        logits = lax.dot_general(
            query, k_ref[:, at], (((1,), (1,)), ((), ())), preferred_element_type=jnp.float32
        ) * HEAD_SIZE ** (-0.5)
        expo = jnp.exp(logits - jnp.max(logits, axis=-1, keepdims=True))
        probs = (expo / jnp.sum(expo, axis=-1, keepdims=True)).astype(jnp.bfloat16)
        out_ref[:, at] = jnp.dot(
            probs, v_ref[:, at], preferred_element_type=jnp.float32
        ).astype(jnp.bfloat16)


def place_kernel(plan, rows, nx, *refs):
    pieces, (out_ref, held) = refs[: len(plan)], refs[len(plan):]
    x = lax.axis_index("mem_1")
    for piece, entries in zip(pieces, plan):
        for begin, length, off_x, row in entries:
            start = lax.rem(x + (off_x % nx), nx) * rows + row
            held[pl.ds(pl.multiple_of(start, 8), length), :] = piece[
                pl.ds(begin, length), :
            ].astype(jnp.float32)
    out_ref[...] = held[...].T.astype(jnp.bfloat16)


def shards(
    tokens,
    query_weight,
    output_weight,
    time_modulation,
    timestep,
    memory_store,
    retrieved,
    fresh_entry,
    write_slot,
):
    nz, nx = lax.axis_size("mem_0"), lax.axis_size("mem_1")
    n_mem = nz * nx
    myself = lax.axis_index(MEM)
    frames = retrieved.shape[0]
    per_frame = n_mem // frames
    stored, _, slots_rows, width = memory_store.shape
    count, model = tokens.shape
    rows = query_weight.shape[0]

    cut = 2 * HEAD_SIZE
    q_a, q_b = query_weight[:, :cut], query_weight[:, cut:]
    qa_x = in_order(around(q_a, "mem_1", True), nx)
    qb_z = in_order(around(q_b, "mem_0", True), nz)
    qa_all = around(qa_x, "mem_0", False)
    qb_all = around(qb_z, "mem_1", False)

    out_t = output_weight.T
    upper = 56
    o_a, o_b = out_t[:upper], out_t[upper:]
    ob_z = lax.all_gather(o_b, "mem_0", axis=0, tiled=False)
    oa_x = in_order(around(o_a, "mem_1", True, -1), nx)
    oa_all = lax.all_gather(oa_x, "mem_0", axis=0, tiled=False)
    ob_all = around(ob_z, "mem_1", False)

    owners = retrieved // stored
    offsets = retrieved % stored
    chosen = jnp.sum(jnp.where(owners == myself, offsets, 0), axis=1)
    picks = (chosen[:, None] * 2 + jnp.arange(per_frame, dtype=jnp.int32)[None]).reshape(-1)
    outgoing = jnp.take(memory_store.reshape(stored * 2, slots_rows, width), picks, axis=0)
    own_fresh = jnp.concatenate([fresh_entry[0], fresh_entry[1]], axis=1)
    extra = own_fresh.shape[1]
    own_fresh = jnp.pad(own_fresh, ((0, 0), (0, HEAD_SIZE - extra)))
    outgoing = jnp.concatenate(
        [outgoing, jnp.broadcast_to(own_fresh, (n_mem, *own_fresh.shape))], axis=2
    )
    incoming = lax.all_to_all(outgoing, MEM, split_axis=0, concat_axis=0, tiled=True)
    my_owners = lax.dynamic_index_in_dim(owners, myself // per_frame, 0, keepdims=False)
    fetched = jnp.take(incoming[:, :, :width], my_owners, axis=0).reshape(-1, width)
    other = lax.ppermute(fetched, "mem_1", [(i, i ^ 1) for i in range(nx)])
    even = myself % 2 == 0
    keys = jnp.where(even, fetched, other)
    vals = jnp.where(even, other, fetched)

    modrow = lax.dynamic_index_in_dim(time_modulation, timestep[0], 0, keepdims=False)
    values = tokens.astype(jnp.float32)
    factor = lax.rsqrt(jnp.mean(values * values, axis=1, keepdims=True) + EPS)
    modulated = (values * factor * (1.0 + modrow[0]) + modrow[1]).astype(jnp.bfloat16)

    pieces, plan = [], []
    for array, off, part in qa_all:
        low = 0 if part is None else part[0]
        pieces.append(array)
        plan.append([(i, off, low + i, 0, cut) for i in range(array.shape[0])])
    for array, off, part in qb_all:
        low = 0 if part is None else part[0]
        pieces.append(array)
        plan.append([(i, low + i, off, cut, width - cut) for i in range(array.shape[0])])
    copies = sum(len(entries) for entries in plan)
    vmem = pl.BlockSpec(memory_space=pltpu.VMEM)
    attended = pl.pallas_call(
        functools.partial(attend_kernel, plan, rows, nz, nx),
        out_shape=jax.ShapeDtypeStruct((count, width), jnp.bfloat16),
        in_specs=[vmem] * 3 + [pl.BlockSpec(memory_space=pl.ANY)] * len(pieces),
        out_specs=vmem,
        scratch_shapes=[
            pltpu.VMEM((model, width), jnp.bfloat16),
            pltpu.VMEM((count, width), jnp.float32),
            pltpu.SemaphoreType.DMA((copies,)),
        ],
        compiler_params=pltpu.CompilerParams(vmem_limit_bytes=40 * 1024 * 1024),
        cost_estimate=pl.CostEstimate(
            flops=2 * count * model * width, bytes_accessed=2 * model * width, transcendentals=0
        ),
        name="query_attend",
    )(modulated, keys, vals, *pieces)

    def term(block):
        return lax.dot_general(
            block, attended, (((block.ndim - 1,), (1,)), ((), ())),
            preferred_element_type=jnp.float32,
        ).astype(jnp.bfloat16)

    (own, _, _), (left, _, _), (right, _, _), (far_0, _, _), (far_1, _, _) = ob_all
    first = jnp.concatenate([term(own), term(left), term(right)], axis=1)
    second = jnp.concatenate(
        [
            term(oa_all.reshape(nz, nx * upper, width)),
            jnp.concatenate([term(far_0), term(far_1)], axis=0),
        ],
        axis=1,
    )
    first = lax.psum_scatter(first, "tp", scatter_dimension=0, tiled=False)
    second = lax.psum_scatter(second, "tp", scatter_dimension=0, tiled=False)
    lower = rows - upper
    places = [
        [(0, lower, 0, upper), (lower, lower, -1, upper), (2 * lower, lower, 1, upper)],
        [(i * upper, upper, i, 0) for i in range(nx)] + [(nx * upper, lower, 2, upper)],
    ]
    memory_out = pl.pallas_call(
        functools.partial(place_kernel, places, rows, nx),
        out_shape=jax.ShapeDtypeStruct((count, width), jnp.bfloat16),
        in_specs=[vmem] * 2,
        out_specs=vmem,
        scratch_shapes=[pltpu.VMEM((width, count), jnp.float32)],
        name="place",
    )(first, second)

    fresh = incoming[:, :, width: width + extra].reshape(n_mem, slots_rows, 2, extra // 2)
    fresh = fresh.transpose(2, 1, 0, 3).reshape(2, slots_rows, width)
    slots = myself * stored + jnp.arange(stored, dtype=jnp.int32)
    updated_store = jnp.where(
        (slots == write_slot[0])[:, None, None, None], fresh[None], memory_store
    )
    return (memory_out, updated_store)


def solution(mesh):
    split = Mesh(mesh.devices.reshape(8, 4, mesh.shape["tp"]), ("mem_0", "mem_1", "tp"))
    in_specs = (
        P(MEM, None),
        P(MEM, "tp"),
        P("tp", MEM),
        P(),
        P(),
        P(MEM, None, None, "tp"),
        P(),
        P(None, None, TP_MEM),
        P(),
    )
    out_specs = (P(MEM, "tp"), P(MEM, None, None, "tp"))
    return jax.shard_map(
        shards, mesh=split, in_specs=in_specs, out_specs=out_specs, check_vma=False
    )
```

```python
import functools

import jax
import jax.numpy as jnp
from jax import lax
from jax.experimental import pallas as pl
from jax.experimental.pallas import tpu as pltpu
from jax.sharding import Mesh
from jax.sharding import PartitionSpec as P

HEAD_SIZE = 128
MEM = ("mem_0", "mem_1")
TP = ("tp_0", "tp_1")
TP_MEM = TP + MEM

EPS = 1e-06


def shift(array, axis, by):
    n = lax.axis_size(axis)
    return lax.ppermute(array, axis, [(i, (i + by) % n) for i in range(n)])


def around(block, axis, whole, direction=1):
    n = lax.axis_size(axis)
    got = [(block, 0, None)]
    fore = back = block
    for step in range(1, (n - 1) // 2 + 1):
        fore, back = shift(fore, axis, 1), shift(back, axis, -1)
        got += [(fore, -step, None), (back, step, None)]
    half = n // 2
    if whole:
        last = shift(fore, axis, 1) if direction > 0 else shift(back, axis, -1)
        got.append((last, half, None))
    else:
        cut = block.shape[0] // 2
        got.append((shift(fore[:cut], axis, 1), half, (0, cut)))
        got.append((shift(back[cut:], axis, -1), half, (cut, block.shape[0])))
    return got


def in_order(got, n):
    return jnp.stack([next(a for a, off, _ in got if off % n == i) for i in range(n)])


def attend_kernel(plan, rows, nz, nx, xm_ref, k_ref, v_ref, *rest):
    pieces, (out_ref, w_ref, acc_ref, sems) = rest[: len(plan)], rest[len(plan):]
    z, x = lax.axis_index("mem_0"), lax.axis_index("mem_1")
    copies = []
    for piece, entries in zip(pieces, plan):
        for index, from_z, at_z, off_x, lane, lanes in entries:
            block_z = lax.rem(z + (at_z % nz), nz) if from_z else at_z
            block = block_z * nx + lax.rem(x + (off_x % nx), nx)
            start = pl.multiple_of(block * rows, 32)
            copy = pltpu.make_async_copy(
                piece.at[index],
                w_ref.at[pl.ds(start, rows), pl.ds(lane, lanes)],
                sems.at[len(copies)],
            )
            copy.start()
            copies.append(copy)
    for copy in copies:
        copy.wait()
    depth = w_ref.shape[0]
    step = depth // 8

    def accumulate(i, carry):
        at = pl.ds(pl.multiple_of(i * step, 128), step)
        acc_ref[...] += jnp.dot(xm_ref[:, at], w_ref[at, :], preferred_element_type=jnp.float32)
        return carry

    acc_ref[...] = jnp.zeros_like(acc_ref)
    lax.fori_loop(0, 8, accumulate, 0)
    for head in range(w_ref.shape[1] // HEAD_SIZE):
        at = pl.ds(head * HEAD_SIZE, HEAD_SIZE)
        query = acc_ref[:, at].astype(jnp.bfloat16)
        logits = lax.dot_general(
            query, k_ref[:, at], (((1,), (1,)), ((), ())), preferred_element_type=jnp.float32
        ) * HEAD_SIZE ** (-0.5)
        expo = jnp.exp(logits - jnp.max(logits, axis=-1, keepdims=True))
        probs = (expo / jnp.sum(expo, axis=-1, keepdims=True)).astype(jnp.bfloat16)
        out_ref[:, at] = jnp.dot(
            probs, v_ref[:, at], preferred_element_type=jnp.float32
        ).astype(jnp.bfloat16)


def place_kernel(offs, nx, *refs):
    pieces, (out_ref, held) = refs[: len(offs)], refs[len(offs):]
    x = lax.axis_index("mem_1")
    for piece, off in zip(pieces, offs):
        rows = piece.shape[0]
        start = lax.rem(x + (off % nx), nx) * rows
        held[pl.ds(pl.multiple_of(start, 32), rows), :] = piece[...].astype(jnp.float32)
    out_ref[...] = held[...].T.astype(jnp.bfloat16)


def shards(
    tokens,
    query_weight,
    output_weight,
    time_modulation,
    timestep,
    memory_store,
    retrieved,
    fresh_entry,
    write_slot,
):
    nz, nx = lax.axis_size("mem_0"), lax.axis_size("mem_1")
    n_mem = nz * nx
    myself = lax.axis_index(MEM)
    frames = retrieved.shape[0]
    per_frame = n_mem // frames
    stored, _, slots_rows, width = memory_store.shape
    count, model = tokens.shape
    rows = query_weight.shape[0]

    cut = 2 * HEAD_SIZE
    q_a, q_b = query_weight[:, :cut], query_weight[:, cut:]
    qa_x = in_order(around(q_a, "mem_1", True), nx)
    qb_z = in_order(around(q_b, "mem_0", True), nz)
    qa_all = lax.all_gather(qa_x, "mem_0", axis=0, tiled=False)
    qb_all = around(qb_z, "mem_1", False)

    o_all, _ = lax.optimization_barrier((output_weight.T, qa_x))
    o_all = lax.all_gather(o_all, "mem_0", axis=0, tiled=False)

    owners = retrieved // stored
    offsets = retrieved % stored
    chosen = jnp.sum(jnp.where(owners == myself, offsets, 0), axis=1)
    picks = (chosen[:, None] * 2 + jnp.arange(per_frame, dtype=jnp.int32)[None]).reshape(-1)
    outgoing = jnp.take(memory_store.reshape(stored * 2, slots_rows, width), picks, axis=0)
    own_fresh = jnp.concatenate([fresh_entry[0], fresh_entry[1]], axis=1)
    extra = own_fresh.shape[1]
    own_fresh = jnp.pad(own_fresh, ((0, 0), (0, HEAD_SIZE - extra)))
    outgoing = jnp.concatenate(
        [outgoing, jnp.broadcast_to(own_fresh, (n_mem, *own_fresh.shape))], axis=2
    )
    outgoing, _ = lax.optimization_barrier((outgoing, qb_z))
    incoming = lax.all_to_all(outgoing, MEM, split_axis=0, concat_axis=0, tiled=True)
    my_owners = lax.dynamic_index_in_dim(owners, myself // per_frame, 0, keepdims=False)
    fetched = jnp.take(incoming[:, :, :width], my_owners, axis=0).reshape(-1, width)
    other = lax.ppermute(fetched, "mem_1", [(i, i ^ 1) for i in range(nx)])
    even = myself % 2 == 0
    keys = jnp.where(even, fetched, other)
    vals = jnp.where(even, other, fetched)

    modrow = lax.dynamic_index_in_dim(time_modulation, timestep[0], 0, keepdims=False)
    values = tokens.astype(jnp.float32)
    factor = lax.rsqrt(jnp.mean(values * values, axis=1, keepdims=True) + EPS)
    modulated = (values * factor * (1.0 + modrow[0]) + modrow[1]).astype(jnp.bfloat16)

    pieces = [qa_all]
    plan = [
        [((i, j), False, i, j, 0, cut) for i in range(nz) for j in range(nx)]
    ]
    for array, off, part in qb_all:
        low = 0 if part is None else part[0]
        pieces.append(array)
        plan.append([(i, True, low + i, off, cut, width - cut) for i in range(array.shape[0])])
    copies = sum(len(entries) for entries in plan)
    vmem = pl.BlockSpec(memory_space=pltpu.VMEM)
    attended = pl.pallas_call(
        functools.partial(attend_kernel, plan, rows, nz, nx),
        out_shape=jax.ShapeDtypeStruct((count, width), jnp.bfloat16),
        in_specs=[vmem] * 3 + [pl.BlockSpec(memory_space=pl.ANY)] * len(pieces),
        out_specs=vmem,
        scratch_shapes=[
            pltpu.VMEM((model, width), jnp.bfloat16),
            pltpu.VMEM((count, width), jnp.float32),
            pltpu.SemaphoreType.DMA((copies,)),
        ],
        compiler_params=pltpu.CompilerParams(vmem_limit_bytes=40 * 1024 * 1024),
        cost_estimate=pl.CostEstimate(
            flops=2 * count * model * width, bytes_accessed=2 * model * width, transcendentals=0
        ),
        name="query_attend",
    )(modulated, keys, vals, *pieces)

    ny, nc = lax.axis_size("tp_0"), lax.axis_size("tp_1")
    core = lax.axis_index("tp_1")
    o_all = o_all.reshape(ny, nc, rows, width)
    o_mine = lax.dynamic_index_in_dim(o_all, core, 1, keepdims=False)
    o_other = lax.dynamic_index_in_dim(o_all, 1 - core, 1, keepdims=False)

    def term(weight, group):
        return lax.dot_general(
            weight, group, (((2,), (1,)), ((), ())), preferred_element_type=jnp.float32
        ).astype(jnp.bfloat16)

    def paired(groups):
        away = jnp.concatenate([term(o_other, group) for group in groups], axis=1)
        came = lax.ppermute(away, "tp_1", [(0, 1), (1, 0)])
        here = jnp.concatenate([term(o_mine, group) for group in groups], axis=1)
        return (here.astype(jnp.float32) + came.astype(jnp.float32)).astype(jnp.bfloat16)

    def summed(pair):
        parts = lax.all_to_all(pair, "tp_0", split_axis=0, concat_axis=0, tiled=True)
        return jnp.sum(parts.astype(jnp.float32), axis=0).astype(jnp.bfloat16)

    (own, _, _), (left, _, _), (right, _, _), (far_0, _, _), (far_1, _, _) = around(
        attended, "mem_1", False
    )
    out_own = summed(paired([own]))
    left, right, out_own = lax.optimization_barrier((left, right, out_own))
    pair_near = paired([left, right])
    far = jnp.concatenate([far_0, far_1], axis=0)
    far, pair_near = lax.optimization_barrier((far, pair_near))
    out_near = summed(pair_near)
    out_far = summed(paired([far]))
    blocks = [
        out_own,
        shift(out_near[:rows], "mem_1", -1),
        shift(out_near[rows:], "mem_1", 1),
        shift(out_far, "mem_1", 2),
    ]
    places = (0, 1, -1, 2)
    memory_out = pl.pallas_call(
        functools.partial(place_kernel, places, nx),
        out_shape=jax.ShapeDtypeStruct((count, width), jnp.bfloat16),
        in_specs=[vmem] * 4,
        out_specs=vmem,
        scratch_shapes=[pltpu.VMEM((width, count), jnp.float32)],
        name="place",
    )(*blocks)

    fresh = incoming[:, :, width: width + extra].reshape(n_mem, slots_rows, 2, extra // 2)
    fresh = fresh.transpose(2, 1, 0, 3).reshape(2, slots_rows, width)
    slots = myself * stored + jnp.arange(stored, dtype=jnp.int32)
    updated_store = jnp.where(
        (slots == write_slot[0])[:, None, None, None], fresh[None], memory_store
    )
    return (memory_out, updated_store)


def solution(mesh):
    split = Mesh(mesh.devices.reshape(8, 4, 4, 2), MEM + TP)
    in_specs = (
        P(MEM, None),
        P(MEM, TP),
        P(TP, MEM),
        P(),
        P(),
        P(MEM, None, None, TP),
        P(),
        P(None, None, TP_MEM),
        P(),
    )
    out_specs = (P(MEM, TP), P(MEM, None, None, TP))
    return jax.shard_map(
        shards, mesh=split, in_specs=in_specs, out_specs=out_specs, check_vma=False
    )
```

```python
import functools

import jax
import jax.numpy as jnp
from jax import lax
from jax.experimental import pallas as pl
from jax.experimental.pallas import tpu as pltpu
from jax.sharding import Mesh
from jax.sharding import PartitionSpec as P

HEAD_SIZE = 128
MEM = ("mem_0", "mem_1")
TP = ("tp_0", "tp_1")
TP_MEM = TP + MEM

EPS = 1e-06


def shift(array, axis, by):
    n = lax.axis_size(axis)
    return lax.ppermute(array, axis, [(i, (i + by) % n) for i in range(n)])


def around(block, axis, whole, direction=1):
    n = lax.axis_size(axis)
    got = [(block, 0, None)]
    fore = back = block
    for step in range(1, (n - 1) // 2 + 1):
        fore, back = shift(fore, axis, 1), shift(back, axis, -1)
        got += [(fore, -step, None), (back, step, None)]
    half = n // 2
    if whole:
        last = shift(fore, axis, 1) if direction > 0 else shift(back, axis, -1)
        got.append((last, half, None))
    else:
        cut = block.shape[0] // 2
        got.append((shift(fore[:cut], axis, 1), half, (0, cut)))
        got.append((shift(back[cut:], axis, -1), half, (cut, block.shape[0])))
    return got


def in_order(got, n):
    return jnp.stack([next(a for a, off, _ in got if off % n == i) for i in range(n)])


def attend_kernel(plan, rows, nx, xm_ref, k_ref, v_ref, *rest):
    pieces, (out_ref, w_ref, acc_ref, sems) = rest[: len(plan)], rest[len(plan):]
    x = lax.axis_index("mem_1")
    copies = []
    for piece, entries in zip(pieces, plan):
        for index, at_z, off_x, row, length in entries:
            block = at_z * nx + lax.rem(x + (off_x % nx), nx)
            start = pl.multiple_of(block * rows + row, 32)
            copy = pltpu.make_async_copy(
                piece.at[index],
                w_ref.at[pl.ds(start, length)],
                sems.at[len(copies)],
            )
            copy.start()
            copies.append(copy)
    for copy in copies:
        copy.wait()
    depth = w_ref.shape[0]
    step = depth // 8

    def accumulate(i, carry):
        at = pl.ds(pl.multiple_of(i * step, 128), step)
        acc_ref[...] += jnp.dot(xm_ref[:, at], w_ref[at, :], preferred_element_type=jnp.float32)
        return carry

    acc_ref[...] = jnp.zeros_like(acc_ref)
    lax.fori_loop(0, 8, accumulate, 0)
    for head in range(w_ref.shape[1] // HEAD_SIZE):
        at = pl.ds(head * HEAD_SIZE, HEAD_SIZE)
        query = acc_ref[:, at].astype(jnp.bfloat16)
        logits = lax.dot_general(
            query, k_ref[:, at], (((1,), (1,)), ((), ())), preferred_element_type=jnp.float32
        ) * HEAD_SIZE ** (-0.5)
        expo = jnp.exp(logits - jnp.max(logits, axis=-1, keepdims=True))
        probs = (expo / jnp.sum(expo, axis=-1, keepdims=True)).astype(jnp.bfloat16)
        out_ref[:, at] = jnp.dot(
            probs, v_ref[:, at], preferred_element_type=jnp.float32
        ).astype(jnp.bfloat16)


def place_kernel(offs, nx, *refs):
    pieces, (out_ref, held) = refs[: len(offs)], refs[len(offs):]
    x = lax.axis_index("mem_1")
    for piece, off in zip(pieces, offs):
        rows = piece.shape[0]
        start = lax.rem(x + (off % nx), nx) * rows
        held[pl.ds(pl.multiple_of(start, 32), rows), :] = piece[...].astype(jnp.float32)
    out_ref[...] = held[...].T.astype(jnp.bfloat16)


def shards(
    tokens,
    query_weight,
    output_weight,
    time_modulation,
    timestep,
    memory_store,
    retrieved,
    fresh_entry,
    write_slot,
):
    nz, nx = lax.axis_size("mem_0"), lax.axis_size("mem_1")
    n_mem = nz * nx
    myself = lax.axis_index(MEM)
    frames = retrieved.shape[0]
    per_frame = n_mem // frames
    stored, _, slots_rows, width = memory_store.shape
    count, model = tokens.shape
    rows = query_weight.shape[0]

    cut = 32
    q_b = lax.all_gather(query_weight[cut:], "mem_0", axis=0, tiled=False)
    q_a = in_order(around(query_weight[:cut], "mem_1", True), nx).reshape(nx * cut, width)
    joint = jnp.concatenate([output_weight.T, q_a], axis=0)
    joint, q_b = lax.optimization_barrier((joint, q_b))
    joint = lax.all_gather(joint, "mem_0", axis=0, tiled=False)
    qb_all = around(q_b, "mem_1", False)

    owners = retrieved // stored
    offsets = retrieved % stored
    chosen = jnp.sum(jnp.where(owners == myself, offsets, 0), axis=1)
    picks = (chosen[:, None] * 2 + jnp.arange(per_frame, dtype=jnp.int32)[None]).reshape(-1)
    outgoing = jnp.take(memory_store.reshape(stored * 2, slots_rows, width), picks, axis=0)
    own_fresh = jnp.concatenate([fresh_entry[0], fresh_entry[1]], axis=1)
    extra = own_fresh.shape[1]
    own_fresh = jnp.pad(own_fresh, ((0, 0), (0, HEAD_SIZE - extra)))
    outgoing = jnp.concatenate(
        [outgoing, jnp.broadcast_to(own_fresh, (n_mem, *own_fresh.shape))], axis=2
    )
    incoming = lax.all_to_all(outgoing, MEM, split_axis=0, concat_axis=0, tiled=True)
    my_owners = lax.dynamic_index_in_dim(owners, myself // per_frame, 0, keepdims=False)
    fetched = jnp.take(incoming[:, :, :width], my_owners, axis=0).reshape(-1, width)
    other = lax.ppermute(fetched, "mem_1", [(i, i ^ 1) for i in range(nx)])
    even = myself % 2 == 0
    keys = jnp.where(even, fetched, other)
    vals = jnp.where(even, other, fetched)

    modrow = lax.dynamic_index_in_dim(time_modulation, timestep[0], 0, keepdims=False)
    values = tokens.astype(jnp.float32)
    factor = lax.rsqrt(jnp.mean(values * values, axis=1, keepdims=True) + EPS)
    modulated = (values * factor * (1.0 + modrow[0]) + modrow[1]).astype(jnp.bfloat16)

    pieces = [joint]
    plan = [
        [
            ((i, pl.ds(rows + j * cut, cut)), i, j, 0, cut)
            for i in range(nz)
            for j in range(nx)
        ]
    ]
    for array, off, part in qb_all:
        low = 0 if part is None else part[0]
        pieces.append(array)
        plan.append([(i, low + i, off, cut, rows - cut) for i in range(array.shape[0])])
    copies = sum(len(entries) for entries in plan)
    vmem = pl.BlockSpec(memory_space=pltpu.VMEM)
    attended = pl.pallas_call(
        functools.partial(attend_kernel, plan, rows, nx),
        out_shape=jax.ShapeDtypeStruct((count, width), jnp.bfloat16),
        in_specs=[vmem] * 3 + [pl.BlockSpec(memory_space=pl.ANY)] * len(pieces),
        out_specs=vmem,
        scratch_shapes=[
            pltpu.VMEM((model, width), jnp.bfloat16),
            pltpu.VMEM((count, width), jnp.float32),
            pltpu.SemaphoreType.DMA((copies,)),
        ],
        compiler_params=pltpu.CompilerParams(vmem_limit_bytes=40 * 1024 * 1024),
        cost_estimate=pl.CostEstimate(
            flops=2 * count * model * width, bytes_accessed=2 * model * width, transcendentals=0
        ),
        name="query_attend",
    )(modulated, keys, vals, *pieces)

    ny, nc = lax.axis_size("tp_0"), lax.axis_size("tp_1")
    core = lax.axis_index("tp_1")
    weight = joint[:, :rows].reshape(ny, nc, rows, width)
    weight = lax.dynamic_slice_in_dim(
        jnp.concatenate([weight, weight], axis=0), lax.axis_index("tp_0"), ny, 0
    )
    mine = lax.dynamic_index_in_dim(weight, core, 1, keepdims=False)
    other = lax.dynamic_index_in_dim(weight, 1 - core, 1, keepdims=False)
    mine, other = lax.optimization_barrier((mine, other))

    def term(weight, group):
        return lax.dot_general(
            weight, group, (((2,), (1,)), ((), ())), preferred_element_type=jnp.float32
        ).astype(jnp.bfloat16)

    def paired(group):
        away = lax.ppermute(term(other, group), "tp_1", [(0, 1), (1, 0)])
        here = term(mine, group)
        pair = (here.astype(jnp.float32) + away.astype(jnp.float32)).astype(jnp.bfloat16)
        return [pair[d] for d in range(ny)]

    def summed(parts):
        parts = [parts[0]] + [shift(parts[d], "tp_0", d) for d in range(1, ny)]
        return sum(part.astype(jnp.float32) for part in parts).astype(jnp.bfloat16)

    own_parts = paired(attended)
    left, right = shift(attended, "mem_1", 1), shift(attended, "mem_1", -1)
    left, right, _ = lax.optimization_barrier((left, right, own_parts))
    far = [shift(left[: count // 2], "mem_1", 1), shift(right[count // 2:], "mem_1", -1)]
    near_parts = paired(jnp.concatenate([left, right], axis=0))
    far, _ = lax.optimization_barrier((far, near_parts))
    far_parts = paired(jnp.concatenate(far, axis=0))
    out_own, near, out_far = summed(own_parts), summed(near_parts), summed(far_parts)
    blocks = [
        out_own,
        shift(near[:, :count], "mem_1", -1),
        shift(near[:, count:], "mem_1", 1),
        shift(out_far, "mem_1", 2),
    ]
    places = (0, 1, -1, 2)
    memory_out = pl.pallas_call(
        functools.partial(place_kernel, places, nx),
        out_shape=jax.ShapeDtypeStruct((count, width), jnp.bfloat16),
        in_specs=[vmem] * 4,
        out_specs=vmem,
        scratch_shapes=[pltpu.VMEM((width, count), jnp.float32)],
        name="place",
    )(*blocks)

    fresh = incoming[:, :, width: width + extra].reshape(n_mem, slots_rows, 2, extra // 2)
    fresh = fresh.transpose(2, 1, 0, 3).reshape(2, slots_rows, width)
    slots = myself * stored + jnp.arange(stored, dtype=jnp.int32)
    updated_store = jnp.where(
        (slots == write_slot[0])[:, None, None, None], fresh[None], memory_store
    )
    return (memory_out, updated_store)


def solution(mesh):
    split = Mesh(mesh.devices.reshape(8, 4, 4, 2), MEM + TP)
    in_specs = (
        P(MEM, None),
        P(MEM, TP),
        P(TP, MEM),
        P(),
        P(),
        P(MEM, None, None, TP),
        P(),
        P(None, None, TP_MEM),
        P(),
    )
    out_specs = (P(MEM, TP), P(MEM, None, None, TP))
    return jax.shard_map(
        shards, mesh=split, in_specs=in_specs, out_specs=out_specs, check_vma=False
    )
```

```python
import functools

import jax
import jax.numpy as jnp
from jax import lax
from jax.experimental import pallas as pl
from jax.experimental.pallas import tpu as pltpu
from jax.sharding import Mesh
from jax.sharding import PartitionSpec as P

HEAD_SIZE = 128
MEM = ("mem_0", "mem_1")
TP = ("tp_0", "tp_1")
TP_MEM = TP + MEM

EPS = 1e-06


def shift(array, axis, by):
    n = lax.axis_size(axis)
    return lax.ppermute(array, axis, [(i, (i + by) % n) for i in range(n)])


def around(block, axis, whole, direction=1):
    n = lax.axis_size(axis)
    got = [(block, 0, None)]
    fore = back = block
    for step in range(1, (n - 1) // 2 + 1):
        fore, back = shift(fore, axis, 1), shift(back, axis, -1)
        got += [(fore, -step, None), (back, step, None)]
    half = n // 2
    if whole:
        last = shift(fore, axis, 1) if direction > 0 else shift(back, axis, -1)
        got.append((last, half, None))
    else:
        cut = block.shape[0] // 2
        got.append((shift(fore[:cut], axis, 1), half, (0, cut)))
        got.append((shift(back[cut:], axis, -1), half, (cut, block.shape[0])))
    return got


def in_order(got, n):
    return jnp.stack([next(a for a, off, _ in got if off % n == i) for i in range(n)])


def attend_kernel(plan, rows, nz, nx, xm_ref, k_ref, v_ref, *rest):
    pieces, (out_ref, w_ref, acc_ref, sems) = rest[: len(plan)], rest[len(plan):]
    z, x = lax.axis_index("mem_0"), lax.axis_index("mem_1")
    copies = []
    for piece, entries in zip(pieces, plan):
        for index, from_z, at_z, off_x, row, length in entries:
            block_z = lax.rem(z + at_z, nz) if from_z else at_z
            block = block_z * nx + lax.rem(x + (off_x % nx), nx)
            start = pl.multiple_of(block * rows + row, 32)
            copy = pltpu.make_async_copy(
                piece.at[index],
                w_ref.at[pl.ds(start, length)],
                sems.at[len(copies)],
            )
            copy.start()
            copies.append(copy)
    for copy in copies:
        copy.wait()
    depth = w_ref.shape[0]
    step = depth // 4

    def accumulate(i, carry):
        at = pl.ds(pl.multiple_of(i * step, 128), step)
        acc_ref[...] += jnp.dot(xm_ref[:, at], w_ref[at, :], preferred_element_type=jnp.float32)
        return carry

    acc_ref[...] = jnp.zeros_like(acc_ref)
    lax.fori_loop(0, 4, accumulate, 0)

    def attend(i, carry):
        part = pl.ds(pl.multiple_of(i * HEAD_SIZE, HEAD_SIZE), HEAD_SIZE)
        for head in range(w_ref.shape[1] // HEAD_SIZE):
            at = pl.ds(head * HEAD_SIZE, HEAD_SIZE)
            query = acc_ref[part, at].astype(jnp.bfloat16)
            logits = lax.dot_general(
                query, k_ref[:, at], (((1,), (1,)), ((), ())), preferred_element_type=jnp.float32
            ) * HEAD_SIZE ** (-0.5)
            expo = jnp.exp(logits - jnp.max(logits, axis=-1, keepdims=True))
            probs = (expo / jnp.sum(expo, axis=-1, keepdims=True)).astype(jnp.bfloat16)
            out_ref[part, at] = jnp.dot(
                probs, v_ref[:, at], preferred_element_type=jnp.float32
            ).astype(jnp.bfloat16)
        return carry

    lax.fori_loop(0, acc_ref.shape[0] // HEAD_SIZE, attend, 0)


def place_kernel(offs, nx, *refs):
    pieces, (out_ref, held) = refs[: len(offs)], refs[len(offs):]
    x = lax.axis_index("mem_1")
    for piece, off in zip(pieces, offs):
        rows = piece.shape[0]
        start = lax.rem(x + (off % nx), nx) * rows
        held[pl.ds(pl.multiple_of(start, 32), rows), :] = piece[...].astype(jnp.float32)
    out_ref[...] = held[...].T.astype(jnp.bfloat16)


def shards(
    tokens,
    query_weight,
    output_weight,
    time_modulation,
    timestep,
    memory_store,
    retrieved,
    fresh_entry,
    write_slot,
):
    nz, nx = lax.axis_size("mem_0"), lax.axis_size("mem_1")
    n_mem = nz * nx
    myself = lax.axis_index(MEM)
    frames = retrieved.shape[0]
    per_frame = n_mem // frames
    stored, _, slots_rows, width = memory_store.shape
    count, model = tokens.shape
    rows = query_weight.shape[0]

    cut = 32
    q_b = in_order(around(query_weight[cut:], "mem_0", True), nz)
    q_a = in_order(around(query_weight[:cut], "mem_1", True), nx).reshape(nx * cut, width)
    joint = jnp.concatenate([output_weight.T, q_a], axis=0)
    joint, q_b = lax.optimization_barrier((joint, q_b))
    joint = lax.all_gather(joint, "mem_0", axis=0, tiled=False)
    qb_all = around(q_b, "mem_1", False)

    owners = retrieved // stored
    offsets = retrieved % stored
    chosen = jnp.sum(jnp.where(owners == myself, offsets, 0), axis=1)
    picks = (chosen[:, None] * 2 + jnp.arange(per_frame, dtype=jnp.int32)[None]).reshape(-1)
    outgoing = jnp.take(memory_store.reshape(stored * 2, slots_rows, width), picks, axis=0)
    own_fresh = jnp.concatenate([fresh_entry[0], fresh_entry[1]], axis=1)
    extra = own_fresh.shape[1]
    own_fresh = jnp.pad(own_fresh, ((0, 0), (0, HEAD_SIZE - extra)))
    outgoing = jnp.concatenate(
        [outgoing, jnp.broadcast_to(own_fresh, (n_mem, *own_fresh.shape))], axis=2
    )
    outgoing, _ = lax.optimization_barrier((outgoing, q_b))
    incoming = lax.all_to_all(outgoing, MEM, split_axis=0, concat_axis=0, tiled=True)
    my_owners = lax.dynamic_index_in_dim(owners, myself // per_frame, 0, keepdims=False)
    fetched = jnp.take(incoming[:, :, :width], my_owners, axis=0).reshape(-1, width)
    other = lax.ppermute(fetched, "mem_1", [(i, i ^ 1) for i in range(nx)])
    even = myself % 2 == 0
    keys = jnp.where(even, fetched, other)
    vals = jnp.where(even, other, fetched)

    modrow = lax.dynamic_index_in_dim(time_modulation, timestep[0], 0, keepdims=False)
    values = tokens.astype(jnp.float32)
    factor = lax.rsqrt(jnp.mean(values * values, axis=1, keepdims=True) + EPS)
    modulated = (values * factor * (1.0 + modrow[0]) + modrow[1]).astype(jnp.bfloat16)

    pieces = [joint]
    plan = [
        [
            ((i, pl.ds(rows + j * cut, cut)), False, i, j, 0, cut)
            for i in range(nz)
            for j in range(nx)
        ]
    ]
    for array, off, part in qb_all:
        low = 0 if part is None else part[0]
        pieces.append(array)
        plan.append([(i, True, low + i, off, cut, rows - cut) for i in range(array.shape[0])])
    copies = sum(len(entries) for entries in plan)
    vmem = pl.BlockSpec(memory_space=pltpu.VMEM)
    attended = pl.pallas_call(
        functools.partial(attend_kernel, plan, rows, nz, nx),
        out_shape=jax.ShapeDtypeStruct((count, width), jnp.bfloat16),
        in_specs=[vmem] * 3 + [pl.BlockSpec(memory_space=pl.ANY)] * len(pieces),
        out_specs=vmem,
        scratch_shapes=[
            pltpu.VMEM((model, width), jnp.bfloat16),
            pltpu.VMEM((count, width), jnp.float32),
            pltpu.SemaphoreType.DMA((copies,)),
        ],
        compiler_params=pltpu.CompilerParams(vmem_limit_bytes=40 * 1024 * 1024),
        cost_estimate=pl.CostEstimate(
            flops=2 * count * model * width, bytes_accessed=2 * model * width, transcendentals=0
        ),
        name="query_attend",
    )(modulated, keys, vals, *pieces)

    ny, nc = lax.axis_size("tp_0"), lax.axis_size("tp_1")
    core = lax.axis_index("tp_1")
    weight = joint[:, :rows].reshape(ny, nc, rows, width)
    weight = lax.dynamic_slice_in_dim(
        jnp.concatenate([weight, weight], axis=0), lax.axis_index("tp_0"), ny, 0
    )
    mine = lax.dynamic_index_in_dim(weight, core, 1, keepdims=False)
    other = lax.dynamic_index_in_dim(weight, 1 - core, 1, keepdims=False)
    swap = [(0, 1), (1, 0)]
    weight = jnp.concatenate([mine, lax.ppermute(other, "tp_1", swap)], axis=2)

    def terms(group):
        away = lax.ppermute(group, "tp_1", swap)
        both = jnp.concatenate([group, away], axis=1)
        return [
            lax.dot_general(
                weight[d], both, (((1,), (1,)), ((), ())), preferred_element_type=jnp.float32
            ).astype(jnp.bfloat16)
            for d in range(ny)
        ]

    def summed(parts):
        parts = [parts[0]] + [shift(parts[d], "tp_0", d) for d in range(1, ny)]
        return sum(part.astype(jnp.float32) for part in parts).astype(jnp.bfloat16)

    left, right = shift(attended, "mem_1", 1), shift(attended, "mem_1", -1)
    own_parts = terms(attended)
    left, right, _ = lax.optimization_barrier((left, right, own_parts))
    far = [shift(left[: count // 2], "mem_1", 1), shift(right[count // 2:], "mem_1", -1)]
    near_parts = terms(jnp.concatenate([left, right], axis=0))
    far, _ = lax.optimization_barrier((far, near_parts))
    far_parts = terms(jnp.concatenate(far, axis=0))
    out_own = summed(own_parts)
    near = summed(near_parts)
    out_far = summed(far_parts)
    blocks = [
        out_own,
        shift(near[:, :count], "mem_1", -1),
        shift(near[:, count:], "mem_1", 1),
        shift(out_far, "mem_1", 2),
    ]
    places = (0, 1, -1, 2)
    memory_out = pl.pallas_call(
        functools.partial(place_kernel, places, nx),
        out_shape=jax.ShapeDtypeStruct((count, width), jnp.bfloat16),
        in_specs=[vmem] * 4,
        out_specs=vmem,
        scratch_shapes=[pltpu.VMEM((width, count), jnp.float32)],
        name="place",
    )(*blocks)

    fresh = incoming[:, :, width: width + extra].reshape(n_mem, slots_rows, 2, extra // 2)
    fresh = fresh.transpose(2, 1, 0, 3).reshape(2, slots_rows, width)
    slots = myself * stored + jnp.arange(stored, dtype=jnp.int32)
    updated_store = jnp.where(
        (slots == write_slot[0])[:, None, None, None], fresh[None], memory_store
    )
    return (memory_out, updated_store)


def solution(mesh):
    split = Mesh(mesh.devices.reshape(8, 4, 4, 2), MEM + TP)
    in_specs = (
        P(MEM, None),
        P(MEM, TP),
        P(TP, MEM),
        P(),
        P(),
        P(MEM, None, None, TP),
        P(),
        P(None, None, TP_MEM),
        P(),
    )
    out_specs = (P(MEM, TP), P(MEM, None, None, TP))
    return jax.shard_map(
        shards, mesh=split, in_specs=in_specs, out_specs=out_specs, check_vma=False
    )
```

```python
import functools

import jax
import jax.numpy as jnp
from jax import lax
from jax.experimental import pallas as pl
from jax.experimental.pallas import tpu as pltpu
from jax.sharding import Mesh
from jax.sharding import PartitionSpec as P

HEAD_SIZE = 128
MEM = ("mem_0", "mem_1")
TP = ("tp_0", "tp_1")
TP_MEM = TP + MEM

EPS = 1e-06


def shift(array, axis, by):
    n = lax.axis_size(axis)
    return lax.ppermute(array, axis, [(i, (i + by) % n) for i in range(n)])


def around(block, axis, whole, direction=1):
    n = lax.axis_size(axis)
    got = [(block, 0, None)]
    fore = back = block
    for step in range(1, (n - 1) // 2 + 1):
        fore, back = shift(fore, axis, 1), shift(back, axis, -1)
        got += [(fore, -step, None), (back, step, None)]
    half = n // 2
    if whole:
        last = shift(fore, axis, 1) if direction > 0 else shift(back, axis, -1)
        got.append((last, half, None))
    else:
        cut = block.shape[0] // 2
        got.append((shift(fore[:cut], axis, 1), half, (0, cut)))
        got.append((shift(back[cut:], axis, -1), half, (cut, block.shape[0])))
    return got


def in_order(got, n):
    return jnp.stack([next(a for a, off, _ in got if off % n == i) for i in range(n)])


def attend_kernel(plan, rows, nx, xm_ref, k_ref, v_ref, *rest):
    pieces, (out_ref, w_ref, acc_ref, sems) = rest[: len(plan)], rest[len(plan):]
    x = lax.axis_index("mem_1")
    copies = []
    for piece, entries in zip(pieces, plan):
        for index, at_z, off_x, lane, lanes in entries:
            block = at_z * nx + lax.rem(x + (off_x % nx), nx)
            start = pl.multiple_of(block * rows, 32)
            copy = pltpu.make_async_copy(
                piece.at[index],
                w_ref.at[pl.ds(start, rows), pl.ds(lane, lanes)],
                sems.at[len(copies)],
            )
            copy.start()
            copies.append(copy)
    for copy in copies:
        copy.wait()
    depth = w_ref.shape[0]
    step = depth // 4

    def accumulate(i, carry):
        at = pl.ds(pl.multiple_of(i * step, 128), step)
        acc_ref[...] += jnp.dot(xm_ref[:, at], w_ref[at, :], preferred_element_type=jnp.float32)
        return carry

    acc_ref[...] = jnp.zeros_like(acc_ref)
    lax.fori_loop(0, 4, accumulate, 0)

    def attend(i, carry):
        part = pl.ds(pl.multiple_of(i * 2 * HEAD_SIZE, HEAD_SIZE), 2 * HEAD_SIZE)
        for head in range(w_ref.shape[1] // HEAD_SIZE):
            at = pl.ds(head * HEAD_SIZE, HEAD_SIZE)
            query = acc_ref[part, at].astype(jnp.bfloat16)
            logits = lax.dot_general(
                query, k_ref[:, at], (((1,), (1,)), ((), ())), preferred_element_type=jnp.float32
            ) * HEAD_SIZE ** (-0.5)
            expo = jnp.exp(logits - jnp.max(logits, axis=-1, keepdims=True))
            probs = (expo / jnp.sum(expo, axis=-1, keepdims=True)).astype(jnp.bfloat16)
            out_ref[part, at] = jnp.dot(
                probs, v_ref[:, at], preferred_element_type=jnp.float32
            ).astype(jnp.bfloat16)
        return carry

    lax.fori_loop(0, acc_ref.shape[0] // (2 * HEAD_SIZE), attend, 0)


def place_kernel(offs, nx, *refs):
    pieces, (out_ref, held) = refs[: len(offs)], refs[len(offs):]
    x = lax.axis_index("mem_1")
    for piece, off in zip(pieces, offs):
        rows = piece.shape[0]
        start = lax.rem(x + (off % nx), nx) * rows
        held[pl.ds(pl.multiple_of(start, 32), rows), :] = piece[...].astype(jnp.float32)
    out_ref[...] = held[...].T.astype(jnp.bfloat16)


def shards(
    tokens,
    query_weight,
    output_weight,
    time_modulation,
    timestep,
    memory_store,
    retrieved,
    fresh_entry,
    write_slot,
):
    nz, nx = lax.axis_size("mem_0"), lax.axis_size("mem_1")
    n_mem = nz * nx
    myself = lax.axis_index(MEM)
    frames = retrieved.shape[0]
    per_frame = n_mem // frames
    stored, _, slots_rows, width = memory_store.shape
    count, model = tokens.shape
    rows = query_weight.shape[0]

    cut = 2 * HEAD_SIZE
    late = width - cut
    joint = jnp.concatenate([query_weight[:, cut:], output_weight.T], axis=1)
    joint = lax.all_gather(joint, "mem_0", axis=0, tiled=False)
    q_a = in_order(around(query_weight[:, :cut], "mem_1", True), nx)
    q_a, joint = lax.optimization_barrier((q_a, joint))
    q_a = lax.all_gather(q_a, "mem_0", axis=0, tiled=False)

    owners = retrieved // stored
    offsets = retrieved % stored
    chosen = jnp.sum(jnp.where(owners == myself, offsets, 0), axis=1)
    picks = (chosen[:, None] * 2 + jnp.arange(per_frame, dtype=jnp.int32)[None]).reshape(-1)
    outgoing = jnp.take(memory_store.reshape(stored * 2, slots_rows, width), picks, axis=0)
    own_fresh = jnp.concatenate([fresh_entry[0], fresh_entry[1]], axis=1)
    extra = own_fresh.shape[1]
    own_fresh = jnp.pad(own_fresh, ((0, 0), (0, HEAD_SIZE - extra)))
    outgoing = jnp.concatenate(
        [outgoing, jnp.broadcast_to(own_fresh, (n_mem, *own_fresh.shape))], axis=2
    )
    incoming = lax.all_to_all(outgoing, MEM, split_axis=0, concat_axis=0, tiled=True)
    my_owners = lax.dynamic_index_in_dim(owners, myself // per_frame, 0, keepdims=False)
    fetched = jnp.take(incoming[:, :, :width], my_owners, axis=0).reshape(-1, width)
    other = lax.ppermute(fetched, "mem_1", [(i, i ^ 1) for i in range(nx)])
    even = myself % 2 == 0
    keys = jnp.where(even, fetched, other)
    vals = jnp.where(even, other, fetched)

    modrow = lax.dynamic_index_in_dim(time_modulation, timestep[0], 0, keepdims=False)
    values = tokens.astype(jnp.float32)
    factor = lax.rsqrt(jnp.mean(values * values, axis=1, keepdims=True) + EPS)
    modulated = (values * factor * (1.0 + modrow[0]) + modrow[1]).astype(jnp.bfloat16)

    joint, modulated, keys, vals = lax.optimization_barrier((joint, modulated, keys, vals))
    qb_all = around(joint[:, :, :late], "mem_1", False)

    fresh = incoming[:, :, width: width + extra].reshape(n_mem, slots_rows, 2, extra // 2)
    fresh = fresh.transpose(2, 1, 0, 3).reshape(2, slots_rows, width)
    slots = myself * stored + jnp.arange(stored, dtype=jnp.int32)
    updated_store = jnp.where(
        (slots == write_slot[0])[:, None, None, None], fresh[None], memory_store
    )

    ny, nc = lax.axis_size("tp_0"), lax.axis_size("tp_1")
    core = lax.axis_index("tp_1")
    weight = joint[:, :, late:].reshape(ny, nc, rows, width)
    weight = lax.dynamic_slice_in_dim(
        jnp.concatenate([weight, weight], axis=0), lax.axis_index("tp_0"), ny, 0
    )
    mine = lax.dynamic_index_in_dim(weight, core, 1, keepdims=False)
    other = lax.dynamic_index_in_dim(weight, 1 - core, 1, keepdims=False)
    modulated, mine, other, updated_store = lax.optimization_barrier(
        (modulated, mine, other, updated_store)
    )

    pieces = [q_a]
    plan = [[((i, j), i, j, 0, cut) for i in range(nz) for j in range(nx)]]
    for array, off, part in qb_all:
        low = 0 if part is None else part[0]
        pieces.append(array)
        plan.append([(i, low + i, off, cut, late) for i in range(array.shape[0])])
    copies = sum(len(entries) for entries in plan)
    vmem = pl.BlockSpec(memory_space=pltpu.VMEM)
    attended = pl.pallas_call(
        functools.partial(attend_kernel, plan, rows, nx),
        out_shape=jax.ShapeDtypeStruct((count, width), jnp.bfloat16),
        in_specs=[vmem] * 3 + [pl.BlockSpec(memory_space=pl.ANY)] * len(pieces),
        out_specs=vmem,
        scratch_shapes=[
            pltpu.VMEM((model, width), jnp.bfloat16),
            pltpu.VMEM((count, width), jnp.float32),
            pltpu.SemaphoreType.DMA((copies,)),
        ],
        compiler_params=pltpu.CompilerParams(vmem_limit_bytes=40 * 1024 * 1024),
        cost_estimate=pl.CostEstimate(
            flops=2 * count * model * width, bytes_accessed=2 * model * width, transcendentals=0
        ),
        name="query_attend",
    )(modulated, keys, vals, *pieces)

    def term(weight, group):
        return lax.dot_general(
            weight, group, (((2,), (1,)), ((), ())), preferred_element_type=jnp.float32
        ).astype(jnp.bfloat16)

    def paired(group):
        away = lax.ppermute(term(other, group), "tp_1", [(0, 1), (1, 0)])
        here = term(mine, group)
        pair = (here.astype(jnp.float32) + away.astype(jnp.float32)).astype(jnp.bfloat16)
        return [pair[d] for d in range(ny)]

    def sent(parts):
        return [parts[0]] + [shift(parts[d], "tp_0", d) for d in range(1, ny)]

    def summed(parts):
        return sum(part.astype(jnp.float32) for part in parts).astype(jnp.bfloat16)

    left, right = shift(attended, "mem_1", 1), shift(attended, "mem_1", -1)
    own_parts = sent(paired(attended))
    far = [shift(left[: count // 2], "mem_1", 1), shift(right[count // 2:], "mem_1", -1)]
    left, right, own_parts = lax.optimization_barrier((left, right, own_parts))
    near_parts = paired(jnp.concatenate([left, right], axis=0))
    far, _ = lax.optimization_barrier((far, near_parts))
    near_parts = sent(near_parts)
    far_parts = sent(paired(jnp.concatenate(far, axis=0)))
    out_own, near, out_far = summed(own_parts), summed(near_parts), summed(far_parts)
    blocks = [
        out_own,
        shift(near[:, :count], "mem_1", -1),
        shift(near[:, count:], "mem_1", 1),
        shift(out_far, "mem_1", 2),
    ]
    places = (0, 1, -1, 2)
    memory_out = pl.pallas_call(
        functools.partial(place_kernel, places, nx),
        out_shape=jax.ShapeDtypeStruct((count, width), jnp.bfloat16),
        in_specs=[vmem] * 4,
        out_specs=vmem,
        scratch_shapes=[pltpu.VMEM((width, count), jnp.float32)],
        name="place",
    )(*blocks)

    return (memory_out, updated_store)


def solution(mesh):
    split = Mesh(mesh.devices.reshape(8, 4, 4, 2), MEM + TP)
    in_specs = (
        P(MEM, None),
        P(MEM, TP),
        P(TP, MEM),
        P(),
        P(),
        P(MEM, None, None, TP),
        P(),
        P(None, None, TP_MEM),
        P(),
    )
    out_specs = (P(MEM, TP), P(MEM, None, None, TP))
    return jax.shard_map(
        shards, mesh=split, in_specs=in_specs, out_specs=out_specs, check_vma=False
    )
```

```python
import functools

import jax
import jax.numpy as jnp
from jax import lax
from jax.experimental import pallas as pl
from jax.experimental.pallas import tpu as pltpu
from jax.sharding import Mesh
from jax.sharding import PartitionSpec as P

HEAD_SIZE = 128
MEM = ("mem_0", "mem_1")
TP = ("tp_0", "tp_1")
TP_MEM = TP + MEM

EPS = 1e-06


def shift(array, axis, by):
    n = lax.axis_size(axis)
    return lax.ppermute(array, axis, [(i, (i + by) % n) for i in range(n)])


def around(block, axis, whole, direction=1):
    n = lax.axis_size(axis)
    got = [(block, 0, None)]
    fore = back = block
    for step in range(1, (n - 1) // 2 + 1):
        fore, back = shift(fore, axis, 1), shift(back, axis, -1)
        got += [(fore, -step, None), (back, step, None)]
    half = n // 2
    if whole:
        last = shift(fore, axis, 1) if direction > 0 else shift(back, axis, -1)
        got.append((last, half, None))
    else:
        cut = block.shape[0] // 2
        got.append((shift(fore[:cut], axis, 1), half, (0, cut)))
        got.append((shift(back[cut:], axis, -1), half, (cut, block.shape[0])))
    return got


def in_order(got, n):
    return jnp.stack([next(a for a, off, _ in got if off % n == i) for i in range(n)])


def attend_kernel(plan, rows, nx, chunks, xm_ref, k_ref, v_ref, *rest):
    pieces, rest = rest[: len(plan)], rest[len(plan):]
    keep_ref, give_ref, x_ref, w_ref, acc_ref, held_ref, x_sems, w_sems = rest
    x, core = lax.axis_index("mem_1"), lax.axis_index("tp_1")
    depth = w_ref.shape[0]
    step = depth // chunks
    entries = [
        (piece, *entry) for piece, part in zip(pieces, plan) for entry in part
    ]
    per_chunk = step // (rows * nx)
    for chunk in range(chunks):
        pltpu.make_async_copy(
            xm_ref.at[:, pl.ds(chunk * step, step)],
            x_ref.at[:, pl.ds(chunk * step, step)],
            x_sems.at[chunk],
        ).start()
        for piece, index, at_z, off_x, lane, lanes in entries:
            if at_z // per_chunk != chunk:
                continue
            block = at_z * nx + lax.rem(x + (off_x % nx), nx)
            start = pl.multiple_of(block * rows, 32)
            pltpu.make_async_copy(
                piece.at[index],
                w_ref.at[pl.ds(start, rows), pl.ds(lane, lanes)],
                w_sems.at[chunk],
            ).start()

    def accumulate(i, carry):
        at = pl.ds(pl.multiple_of(i * step, 128), step)
        pltpu.make_async_copy(x_ref.at[:, at], x_ref.at[:, at], x_sems.at[i]).wait()
        pltpu.make_async_copy(w_ref.at[at, :], w_ref.at[at, :], w_sems.at[i]).wait()
        acc_ref[...] += jnp.dot(x_ref[:, at], w_ref[at, :], preferred_element_type=jnp.float32)
        return carry

    acc_ref[...] = jnp.zeros_like(acc_ref)
    lax.fori_loop(0, chunks, accumulate, 0)
    half = acc_ref.shape[0] // 2

    def attend(i, carry):
        part = pl.ds(pl.multiple_of(i * half, half), half)
        for head in range(w_ref.shape[1] // HEAD_SIZE):
            at = pl.ds(head * HEAD_SIZE, HEAD_SIZE)
            query = acc_ref[part, at].astype(jnp.bfloat16)
            logits = lax.dot_general(
                query, k_ref[:, at], (((1,), (1,)), ((), ())), preferred_element_type=jnp.float32
            ) * HEAD_SIZE ** (-0.5)
            expo = jnp.exp(logits - jnp.max(logits, axis=-1, keepdims=True))
            probs = (expo / jnp.sum(expo, axis=-1, keepdims=True)).astype(jnp.bfloat16)
            held_ref[part, at] = jnp.dot(
                probs, v_ref[:, at], preferred_element_type=jnp.float32
            ).astype(jnp.bfloat16)
        return carry

    lax.fori_loop(0, 2, attend, 0)
    keep_ref[...] = held_ref[pl.ds(pl.multiple_of(core * half, half), half), :]
    give_ref[...] = held_ref[pl.ds(pl.multiple_of((1 - core) * half, half), half), :]


def place_kernel(offs, nx, *refs):
    pieces, (out_ref, held) = refs[: len(offs)], refs[len(offs):]
    x, core = lax.axis_index("mem_1"), lax.axis_index("tp_1")
    half = out_ref.shape[0] // 2
    for same in range(2):
        for piece, (off, mine) in zip(pieces, offs):
            if mine == same:
                rows = piece.shape[0]
                start = lax.rem(x + (off % nx), nx) * rows
                held[pl.ds(pl.multiple_of(start, 32), rows), :] = piece[...].astype(jnp.float32)
        to = core if same else 1 - core
        out_ref[pl.ds(pl.multiple_of(to * half, half), half), :] = held[...].T.astype(jnp.bfloat16)


def shards(
    tokens,
    query_weight,
    output_weight,
    time_modulation,
    timestep,
    memory_store,
    retrieved,
    fresh_entry,
    write_slot,
):
    nz, nx = lax.axis_size("mem_0"), lax.axis_size("mem_1")
    n_mem = nz * nx
    myself = lax.axis_index(MEM)
    frames = retrieved.shape[0]
    per_frame = n_mem // frames
    stored, _, slots_rows, width = memory_store.shape
    count, model = tokens.shape
    rows = query_weight.shape[0]

    cut = 2 * HEAD_SIZE
    late = width - cut
    joint = jnp.concatenate([query_weight[:, cut:], output_weight.T], axis=1)
    joint = lax.all_gather(joint, "mem_0", axis=0, tiled=False)
    q_a = in_order(around(query_weight[:, :cut], "mem_1", True), nx)
    q_a, joint = lax.optimization_barrier((q_a, joint))
    q_a = lax.all_gather(q_a, "mem_0", axis=0, tiled=False)

    owners = retrieved // stored
    offsets = retrieved % stored
    chosen = jnp.sum(jnp.where(owners == myself, offsets, 0), axis=1)
    picks = (chosen[:, None] * 2 + jnp.arange(per_frame, dtype=jnp.int32)[None]).reshape(-1)
    outgoing = jnp.take(memory_store.reshape(stored * 2, slots_rows, width), picks, axis=0)
    own_fresh = jnp.concatenate([fresh_entry[0], fresh_entry[1]], axis=1)
    extra = own_fresh.shape[1]
    own_fresh = jnp.pad(own_fresh, ((0, 0), (0, HEAD_SIZE - extra)))
    outgoing = jnp.concatenate(
        [outgoing, jnp.broadcast_to(own_fresh, (n_mem, *own_fresh.shape))], axis=2
    )
    incoming = lax.all_to_all(outgoing, MEM, split_axis=0, concat_axis=0, tiled=True)
    my_owners = lax.dynamic_index_in_dim(owners, myself // per_frame, 0, keepdims=False)
    fetched = jnp.take(incoming[:, :, :width], my_owners, axis=0).reshape(-1, width)
    other = lax.ppermute(fetched, "mem_1", [(i, i ^ 1) for i in range(nx)])
    even = myself % 2 == 0
    keys = jnp.where(even, fetched, other)
    vals = jnp.where(even, other, fetched)

    modrow = lax.dynamic_index_in_dim(time_modulation, timestep[0], 0, keepdims=False)
    values = tokens.astype(jnp.float32)
    factor = lax.rsqrt(jnp.mean(values * values, axis=1, keepdims=True) + EPS)
    modulated = (values * factor * (1.0 + modrow[0]) + modrow[1]).astype(jnp.bfloat16)

    joint, modulated, keys, vals = lax.optimization_barrier((joint, modulated, keys, vals))
    own = joint[:, :, :late]
    fore, back = shift(own, "mem_1", 1), shift(own, "mem_1", -1)
    low, high = shift(fore[: nz // 2], "mem_1", 1), shift(back[nz // 2:], "mem_1", -1)
    qb_all = ((own, 0, 0), (fore, -1, 0), (back, 1, 0), (low, 2, 0), (high, 2, nz // 2))

    fresh = incoming[:, :, width: width + extra].reshape(n_mem, slots_rows, 2, extra // 2)
    fresh = fresh.transpose(2, 1, 0, 3).reshape(2, slots_rows, width)
    slots = myself * stored + jnp.arange(stored, dtype=jnp.int32)
    updated_store = jnp.where(
        (slots == write_slot[0])[:, None, None, None], fresh[None], memory_store
    )

    ny, nc = lax.axis_size("tp_0"), lax.axis_size("tp_1")
    core = lax.axis_index("tp_1")
    swap = [(0, 1), (1, 0)]
    weight = joint[:, :, late:]
    away = lax.ppermute(weight, "tp_1", swap)
    weight = jnp.concatenate([weight, away], axis=2)
    weight = weight.reshape(ny, nc, rows, 2 * width)
    weight = lax.dynamic_slice_in_dim(
        jnp.concatenate([weight, weight], axis=0), lax.axis_index("tp_0"), ny, 0
    )
    weight = jnp.concatenate(
        [
            lax.dynamic_index_in_dim(weight, core, 1, keepdims=False),
            lax.dynamic_index_in_dim(weight, 1 - core, 1, keepdims=False),
        ],
        axis=1,
    )
    modulated, weight, updated_store = lax.optimization_barrier(
        (modulated, weight, updated_store)
    )

    pieces = [q_a]
    plan = [[((i, j), i, j, 0, cut) for i in range(nz) for j in range(nx)]]
    for array, off, low in qb_all:
        pieces.append(array)
        plan.append([(i, low + i, off, cut, late) for i in range(array.shape[0])])
    chunks = 4
    vmem = pl.BlockSpec(memory_space=pltpu.VMEM)
    hbm = pl.BlockSpec(memory_space=pltpu.HBM)
    half = jax.ShapeDtypeStruct((count // 2, width), jnp.bfloat16)
    keep, give = pl.pallas_call(
        functools.partial(attend_kernel, plan, rows, nx, chunks),
        out_shape=(half, half),
        in_specs=[hbm, vmem, vmem] + [hbm] * len(pieces),
        out_specs=(vmem, vmem),
        scratch_shapes=[
            pltpu.VMEM((count, model), jnp.bfloat16),
            pltpu.VMEM((model, width), jnp.bfloat16),
            pltpu.VMEM((count, width), jnp.float32),
            pltpu.VMEM((count, width), jnp.bfloat16),
            pltpu.SemaphoreType.DMA((chunks,)),
            pltpu.SemaphoreType.DMA((chunks,)),
        ],
        compiler_params=pltpu.CompilerParams(vmem_limit_bytes=40 * 1024 * 1024),
        cost_estimate=pl.CostEstimate(
            flops=2 * count * model * width, bytes_accessed=2 * model * width, transcendentals=0
        ),
        name="query_attend",
    )(modulated, keys, vals, *pieces)

    attended = jnp.concatenate([keep, lax.ppermute(give, "tp_1", swap)], axis=1)

    def terms(group):
        return [
            lax.dot_general(
                weight[d], group, (((1,), (1,)), ((), ())), preferred_element_type=jnp.float32
            ).astype(jnp.bfloat16)
            for d in range(ny)
        ]

    def sent(parts):
        return [parts[0]] + [shift(parts[d], "tp_0", d) for d in range(1, ny)]

    def summed(parts):
        total = sum(part.astype(jnp.float32) for part in parts).astype(jnp.bfloat16)
        return total[:rows], total[rows:]

    def returned(block, by, mine):
        pairs = [
            (i * nc + c, (i + by) % nx * nc + (c if mine else 1 - c))
            for i in range(nx)
            for c in range(nc)
        ]
        return lax.ppermute(block, ("mem_1", "tp_1"), pairs)

    left, right = shift(attended, "mem_1", 1), shift(attended, "mem_1", -1)
    own_parts = sent(terms(attended))
    quarter = count // 4
    far = [shift(left[:quarter], "mem_1", 1), shift(right[quarter:], "mem_1", -1)]
    near_parts = sent(terms(jnp.concatenate([left, right], axis=0)))
    far_parts = sent(terms(jnp.concatenate(far, axis=0)))
    blocks, places = [], []
    for parts, bys in ((own_parts, (0,)), (near_parts, (-1, 1)), (far_parts, (2,))):
        both = summed(parts)
        for i, by in enumerate(bys):
            for mine in (1, 0):
                block = both[1 - mine][:, i * 2 * quarter: (i + 1) * 2 * quarter]
                blocks.append(block if mine and not by else returned(block, by, mine))
                places.append((-by, mine))
    memory_out = pl.pallas_call(
        functools.partial(place_kernel, places, nx),
        out_shape=jax.ShapeDtypeStruct((count, width), jnp.bfloat16),
        in_specs=[vmem] * len(blocks),
        out_specs=vmem,
        scratch_shapes=[pltpu.VMEM((width, count // 2), jnp.float32)],
        name="place",
    )(*blocks)

    return (memory_out, updated_store)


def solution(mesh):
    split = Mesh(mesh.devices.reshape(8, 4, 4, 2), MEM + TP)
    in_specs = (
        P(MEM, None),
        P(MEM, TP),
        P(TP, MEM),
        P(),
        P(),
        P(MEM, None, None, TP),
        P(),
        P(None, None, TP_MEM),
        P(),
    )
    out_specs = (P(MEM, TP), P(MEM, None, None, TP))
    return jax.shard_map(
        shards, mesh=split, in_specs=in_specs, out_specs=out_specs, check_vma=False
    )
```

```python
import functools

import jax
import jax.numpy as jnp
from jax import lax
from jax.experimental import pallas as pl
from jax.experimental.pallas import tpu as pltpu
from jax.sharding import Mesh
from jax.sharding import PartitionSpec as P

HEAD_SIZE = 128
MEM = ("mem_0", "mem_1")
TP = ("tp_0", "tp_1")
TP_MEM = TP + MEM

EPS = 1e-06


def shift(array, axis, by):
    n = lax.axis_size(axis)
    return lax.ppermute(array, axis, [(i, (i + by) % n) for i in range(n)])


def around(block, axis, whole, direction=1):
    n = lax.axis_size(axis)
    got = [(block, 0, None)]
    fore = back = block
    for step in range(1, (n - 1) // 2 + 1):
        fore, back = shift(fore, axis, 1), shift(back, axis, -1)
        got += [(fore, -step, None), (back, step, None)]
    half = n // 2
    if whole:
        last = shift(fore, axis, 1) if direction > 0 else shift(back, axis, -1)
        got.append((last, half, None))
    else:
        cut = block.shape[0] // 2
        got.append((shift(fore[:cut], axis, 1), half, (0, cut)))
        got.append((shift(back[cut:], axis, -1), half, (cut, block.shape[0])))
    return got


def in_order(got, n):
    return jnp.stack([next(a for a, off, _ in got if off % n == i) for i in range(n)])


def attend_kernel(plan, rows, nx, chunks, xm_ref, k_ref, v_ref, *rest):
    pieces, rest = rest[: len(plan)], rest[len(plan):]
    keep_ref, give_ref, x_ref, w_ref, acc_ref, held_ref, x_sems, w_sems = rest
    x, core = lax.axis_index("mem_1"), lax.axis_index("tp_1")
    depth = w_ref.shape[0]
    step = depth // chunks
    entries = [
        (piece, *entry) for piece, part in zip(pieces, plan) for entry in part
    ]
    per_chunk = step // (rows * nx)
    for chunk in range(chunks):
        pltpu.make_async_copy(
            xm_ref.at[:, pl.ds(chunk * step, step)],
            x_ref.at[:, pl.ds(chunk * step, step)],
            x_sems.at[chunk],
        ).start()
        for piece, index, at_z, off_x, lane, lanes in entries:
            if at_z // per_chunk != chunk:
                continue
            block = at_z * nx + lax.rem(x + (off_x % nx), nx)
            start = pl.multiple_of(block * rows, 32)
            pltpu.make_async_copy(
                piece.at[index],
                w_ref.at[pl.ds(start, rows), pl.ds(lane, lanes)],
                w_sems.at[chunk],
            ).start()

    def accumulate(i, carry):
        at = pl.ds(pl.multiple_of(i * step, 128), step)
        pltpu.make_async_copy(x_ref.at[:, at], x_ref.at[:, at], x_sems.at[i]).wait()
        pltpu.make_async_copy(w_ref.at[at, :], w_ref.at[at, :], w_sems.at[i]).wait()
        acc_ref[...] += jnp.dot(x_ref[:, at], w_ref[at, :], preferred_element_type=jnp.float32)
        return carry

    acc_ref[...] = jnp.zeros_like(acc_ref)
    lax.fori_loop(0, chunks, accumulate, 0)
    half = acc_ref.shape[0] // 2

    def attend(i, carry):
        part = pl.ds(pl.multiple_of(i * half, half), half)
        for head in range(w_ref.shape[1] // HEAD_SIZE):
            at = pl.ds(head * HEAD_SIZE, HEAD_SIZE)
            query = acc_ref[part, at].astype(jnp.bfloat16)
            logits = lax.dot_general(
                query, k_ref[:, at], (((1,), (1,)), ((), ())), preferred_element_type=jnp.float32
            ) * HEAD_SIZE ** (-0.5)
            expo = jnp.exp(logits - jnp.max(logits, axis=-1, keepdims=True))
            probs = (expo / jnp.sum(expo, axis=-1, keepdims=True)).astype(jnp.bfloat16)
            held_ref[part, at] = jnp.dot(
                probs, v_ref[:, at], preferred_element_type=jnp.float32
            ).astype(jnp.bfloat16)
        return carry

    lax.fori_loop(0, 2, attend, 0)
    keep_ref[...] = held_ref[pl.ds(pl.multiple_of(core * half, half), half), :]
    give_ref[...] = held_ref[pl.ds(pl.multiple_of((1 - core) * half, half), half), :]


def place_kernel(offs, nx, *refs):
    pieces, (out_ref, held) = refs[: len(offs)], refs[len(offs):]
    x, core = lax.axis_index("mem_1"), lax.axis_index("tp_1")
    half = out_ref.shape[0] // 2
    for same in range(2):
        for piece, (off, mine) in zip(pieces, offs):
            if mine == same:
                rows = piece.shape[0]
                start = lax.rem(x + (off % nx), nx) * rows
                held[pl.ds(pl.multiple_of(start, 32), rows), :] = piece[...].astype(jnp.float32)
        to = core if same else 1 - core
        out_ref[pl.ds(pl.multiple_of(to * half, half), half), :] = held[...].T.astype(jnp.bfloat16)


def shards(
    tokens,
    query_weight,
    output_weight,
    time_modulation,
    timestep,
    memory_store,
    retrieved,
    fresh_entry,
    write_slot,
):
    nz, nx = lax.axis_size("mem_0"), lax.axis_size("mem_1")
    n_mem = nz * nx
    myself = lax.axis_index(MEM)
    frames = retrieved.shape[0]
    per_frame = n_mem // frames
    stored, _, slots_rows, width = memory_store.shape
    count, model = tokens.shape
    rows = query_weight.shape[0]

    cut = 2 * HEAD_SIZE
    late = width - cut
    joint = jnp.concatenate([query_weight[:, cut:], output_weight.T], axis=1)
    joint = lax.all_gather(joint, "mem_0", axis=0, tiled=False)
    q_a = in_order(around(query_weight[:, :cut], "mem_1", True), nx)
    q_a, joint = lax.optimization_barrier((q_a, joint))
    q_a = lax.all_gather(q_a, "mem_0", axis=0, tiled=False)

    owners = retrieved // stored
    offsets = retrieved % stored
    chosen = jnp.sum(jnp.where(owners == myself, offsets, 0), axis=1)
    picks = (chosen[:, None] * 2 + jnp.arange(per_frame, dtype=jnp.int32)[None]).reshape(-1)
    outgoing = jnp.take(memory_store.reshape(stored * 2, slots_rows, width), picks, axis=0)
    own_fresh = jnp.concatenate([fresh_entry[0], fresh_entry[1]], axis=1)
    extra = own_fresh.shape[1]
    own_fresh = jnp.pad(own_fresh, ((0, 0), (0, HEAD_SIZE - extra)))
    outgoing = jnp.concatenate(
        [outgoing, jnp.broadcast_to(own_fresh, (n_mem, *own_fresh.shape))], axis=2
    )
    incoming = lax.all_to_all(outgoing, MEM, split_axis=0, concat_axis=0, tiled=True)
    my_owners = lax.dynamic_index_in_dim(owners, myself // per_frame, 0, keepdims=False)
    fetched = jnp.take(incoming[:, :, :width], my_owners, axis=0).reshape(-1, width)
    other = lax.ppermute(fetched, "mem_1", [(i, i ^ 1) for i in range(nx)])
    even = myself % 2 == 0
    keys = jnp.where(even, fetched, other)
    vals = jnp.where(even, other, fetched)

    modrow = lax.dynamic_index_in_dim(time_modulation, timestep[0], 0, keepdims=False)
    values = tokens.astype(jnp.float32)
    factor = lax.rsqrt(jnp.mean(values * values, axis=1, keepdims=True) + EPS)
    modulated = (values * factor * (1.0 + modrow[0]) + modrow[1]).astype(jnp.bfloat16)

    joint, modulated, keys, vals = lax.optimization_barrier((joint, modulated, keys, vals))
    own = joint[:, :, :late]
    fore, back = shift(own, "mem_1", 1), shift(own, "mem_1", -1)
    low, high = shift(fore[: nz // 2], "mem_1", 1), shift(back[nz // 2:], "mem_1", -1)
    qb_all = ((own, 0, 0), (fore, -1, 0), (back, 1, 0), (low, 2, 0), (high, 2, nz // 2))

    fresh = incoming[:, :, width: width + extra].reshape(n_mem, slots_rows, 2, extra // 2)
    fresh = fresh.transpose(2, 1, 0, 3).reshape(2, slots_rows, width)
    slots = myself * stored + jnp.arange(stored, dtype=jnp.int32)
    updated_store = jnp.where(
        (slots == write_slot[0])[:, None, None, None], fresh[None], memory_store
    )

    ny, nc = lax.axis_size("tp_0"), lax.axis_size("tp_1")
    core = lax.axis_index("tp_1")
    swap = [(0, 1), (1, 0)]
    weight = joint[:, :, late:]
    away = lax.ppermute(weight, "tp_1", swap)
    weight = jnp.concatenate([weight, away], axis=2)
    weight = weight.reshape(ny, nc, rows, 2 * width)
    weight = lax.dynamic_slice_in_dim(
        jnp.concatenate([weight, weight], axis=0), lax.axis_index("tp_0"), ny, 0
    )
    weight = jnp.concatenate(
        [
            lax.dynamic_index_in_dim(weight, core, 1, keepdims=False),
            lax.dynamic_index_in_dim(weight, 1 - core, 1, keepdims=False),
        ],
        axis=1,
    )
    modulated, weight, updated_store = lax.optimization_barrier(
        (modulated, weight, updated_store)
    )

    pieces = [q_a]
    plan = [[((i, j), i, j, 0, cut) for i in range(nz) for j in range(nx)]]
    for array, off, low in qb_all:
        pieces.append(array)
        plan.append([(i, low + i, off, cut, late) for i in range(array.shape[0])])
    chunks = 4
    vmem = pl.BlockSpec(memory_space=pltpu.VMEM)
    hbm = pl.BlockSpec(memory_space=pltpu.HBM)
    half = jax.ShapeDtypeStruct((count // 2, width), jnp.bfloat16)
    keep, give = pl.pallas_call(
        functools.partial(attend_kernel, plan, rows, nx, chunks),
        out_shape=(half, half),
        in_specs=[hbm, vmem, vmem] + [hbm] * len(pieces),
        out_specs=(vmem, vmem),
        scratch_shapes=[
            pltpu.VMEM((count, model), jnp.bfloat16),
            pltpu.VMEM((model, width), jnp.bfloat16),
            pltpu.VMEM((count, width), jnp.float32),
            pltpu.VMEM((count, width), jnp.bfloat16),
            pltpu.SemaphoreType.DMA((chunks,)),
            pltpu.SemaphoreType.DMA((chunks,)),
        ],
        compiler_params=pltpu.CompilerParams(vmem_limit_bytes=62 * 1024 * 1024),
        cost_estimate=pl.CostEstimate(
            flops=2 * count * model * width, bytes_accessed=2 * model * width, transcendentals=0
        ),
        name="query_attend",
    )(modulated, keys, vals, *pieces)

    attended = jnp.concatenate([keep, lax.ppermute(give, "tp_1", swap)], axis=1)

    def term(d, group):
        return lax.dot_general(
            weight[d], group, (((1,), (1,)), ((), ())), preferred_element_type=jnp.float32
        ).astype(jnp.bfloat16)

    def terms(group):
        home = term(0, group)
        return [home] + [term(d, group) for d in range(1, ny)]

    def sent(parts):
        return [parts[0]] + [shift(parts[d], "tp_0", d) for d in range(1, ny)]

    def summed(parts):
        total = sum(part.astype(jnp.float32) for part in parts).astype(jnp.bfloat16)
        return total[:rows], total[rows:]

    def returned(block, by, mine):
        pairs = [
            (i * nc + c, (i + by) % nx * nc + (c if mine else 1 - c))
            for i in range(nx)
            for c in range(nc)
        ]
        return lax.ppermute(block, ("mem_1", "tp_1"), pairs)

    left, right = shift(attended, "mem_1", 1), shift(attended, "mem_1", -1)
    own_parts = sent(terms(attended))
    quarter = count // 4
    far = [shift(left[:quarter], "mem_1", 1), shift(right[quarter:], "mem_1", -1)]
    near_parts = sent(terms(jnp.concatenate([left, right], axis=0)))
    far_parts = sent(terms(jnp.concatenate(far, axis=0)))
    blocks, places = [], []
    groups = ((own_parts, (0,)), (near_parts, (-1, 1)), (far_parts, (2,)))
    for parts, bys in groups:
        both = summed(parts)
        for i, by in enumerate(bys):
            for mine in (1, 0):
                block = both[1 - mine][:, i * 2 * quarter: (i + 1) * 2 * quarter]
                blocks.append(block if mine and not by else returned(block, by, mine))
                places.append((-by, mine))
    memory_out = pl.pallas_call(
        functools.partial(place_kernel, places, nx),
        out_shape=jax.ShapeDtypeStruct((count, width), jnp.bfloat16),
        in_specs=[vmem] * len(blocks),
        out_specs=vmem,
        scratch_shapes=[pltpu.VMEM((width, count // 2), jnp.float32)],
        name="place",
    )(*blocks)

    return (memory_out, updated_store)


def solution(mesh):
    split = Mesh(mesh.devices.reshape(8, 4, 4, 2), MEM + TP)
    in_specs = (
        P(MEM, None),
        P(MEM, TP),
        P(TP, MEM),
        P(),
        P(),
        P(MEM, None, None, TP),
        P(),
        P(None, None, TP_MEM),
        P(),
    )
    out_specs = (P(MEM, TP), P(MEM, None, None, TP))
    return jax.shard_map(
        shards, mesh=split, in_specs=in_specs, out_specs=out_specs, check_vma=False
    )
```

```python
import functools

import jax
import jax.numpy as jnp
from jax import lax
from jax.experimental import pallas as pl
from jax.experimental.pallas import tpu as pltpu
from jax.sharding import Mesh
from jax.sharding import PartitionSpec as P

HEAD_SIZE = 128
MEM = ("mem_0", "mem_1")
TP = ("tp_0", "tp_1")
TP_MEM = TP + MEM

EPS = 1e-06


def shift(array, axis, by):
    n = lax.axis_size(axis)
    return lax.ppermute(array, axis, [(i, (i + by) % n) for i in range(n)])


def around(block, axis, whole, direction=1):
    n = lax.axis_size(axis)
    got = [(block, 0, None)]
    fore = back = block
    for step in range(1, (n - 1) // 2 + 1):
        fore, back = shift(fore, axis, 1), shift(back, axis, -1)
        got += [(fore, -step, None), (back, step, None)]
    half = n // 2
    if whole:
        last = shift(fore, axis, 1) if direction > 0 else shift(back, axis, -1)
        got.append((last, half, None))
    else:
        cut = block.shape[0] // 2
        got.append((shift(fore[:cut], axis, 1), half, (0, cut)))
        got.append((shift(back[cut:], axis, -1), half, (cut, block.shape[0])))
    return got


def in_order(got, n):
    return jnp.stack([next(a for a, off, _ in got if off % n == i) for i in range(n)])


def join_kernel(cut, q_ref, o_ref, early_ref, joint_ref):
    early_ref[...] = q_ref[:, :cut]
    joint_ref[:, : q_ref.shape[1] - cut] = q_ref[:, cut:]
    joint_ref[:, q_ref.shape[1] - cut:] = o_ref[...]


def attend_kernel(plan, rows, nx, chunks, xm_ref, k_ref, v_ref, *rest):
    pieces, rest = rest[: len(plan)], rest[len(plan):]
    keep_ref, give_ref, x_ref, w_ref, acc_ref, held_ref, x_sems, w_sems = rest
    x, core = lax.axis_index("mem_1"), lax.axis_index("tp_1")
    depth = w_ref.shape[0]
    step = depth // chunks
    entries = [
        (piece, *entry) for piece, part in zip(pieces, plan) for entry in part
    ]
    per_chunk = step // (rows * nx)
    for chunk in range(chunks):
        pltpu.make_async_copy(
            xm_ref.at[:, pl.ds(chunk * step, step)],
            x_ref.at[:, pl.ds(chunk * step, step)],
            x_sems.at[chunk],
        ).start()
        for piece, index, at_z, off_x, lane, lanes in entries:
            if at_z // per_chunk != chunk:
                continue
            block = at_z * nx + lax.rem(x + (off_x % nx), nx)
            start = pl.multiple_of(block * rows, 32)
            pltpu.make_async_copy(
                piece.at[index],
                w_ref.at[pl.ds(start, rows), pl.ds(lane, lanes)],
                w_sems.at[chunk],
            ).start()

    def accumulate(i, carry):
        at = pl.ds(pl.multiple_of(i * step, 128), step)
        pltpu.make_async_copy(x_ref.at[:, at], x_ref.at[:, at], x_sems.at[i]).wait()
        pltpu.make_async_copy(w_ref.at[at, :], w_ref.at[at, :], w_sems.at[i]).wait()
        acc_ref[...] += jnp.dot(x_ref[:, at], w_ref[at, :], preferred_element_type=jnp.float32)
        return carry

    acc_ref[...] = jnp.zeros_like(acc_ref)
    lax.fori_loop(0, chunks, accumulate, 0)
    half = acc_ref.shape[0] // 2

    def attend(i, carry):
        part = pl.ds(pl.multiple_of(i * half, half), half)
        for head in range(w_ref.shape[1] // HEAD_SIZE):
            at = pl.ds(head * HEAD_SIZE, HEAD_SIZE)
            query = acc_ref[part, at].astype(jnp.bfloat16)
            logits = lax.dot_general(
                query, k_ref[:, at], (((1,), (1,)), ((), ())), preferred_element_type=jnp.float32
            ) * HEAD_SIZE ** (-0.5)
            expo = jnp.exp(logits - jnp.max(logits, axis=-1, keepdims=True))
            probs = (expo / jnp.sum(expo, axis=-1, keepdims=True)).astype(jnp.bfloat16)
            held_ref[part, at] = jnp.dot(
                probs, v_ref[:, at], preferred_element_type=jnp.float32
            ).astype(jnp.bfloat16)
        return carry

    lax.fori_loop(0, 2, attend, 0)
    keep_ref[...] = held_ref[pl.ds(pl.multiple_of(core * half, half), half), :]
    give_ref[...] = held_ref[pl.ds(pl.multiple_of((1 - core) * half, half), half), :]


def place_kernel(offs, nx, *refs):
    pieces, (out_ref, held) = refs[: len(offs)], refs[len(offs):]
    x, core = lax.axis_index("mem_1"), lax.axis_index("tp_1")
    half = out_ref.shape[0] // 2
    for same in range(2):
        for piece, (off, mine) in zip(pieces, offs):
            if mine == same:
                rows = piece.shape[0]
                start = lax.rem(x + (off % nx), nx) * rows
                held[pl.ds(pl.multiple_of(start, 32), rows), :] = piece[...].astype(jnp.float32)
        to = core if same else 1 - core
        out_ref[pl.ds(pl.multiple_of(to * half, half), half), :] = held[...].T.astype(jnp.bfloat16)


def shards(
    tokens,
    query_weight,
    output_weight,
    time_modulation,
    timestep,
    memory_store,
    retrieved,
    fresh_entry,
    write_slot,
):
    nz, nx = lax.axis_size("mem_0"), lax.axis_size("mem_1")
    n_mem = nz * nx
    myself = lax.axis_index(MEM)
    frames = retrieved.shape[0]
    per_frame = n_mem // frames
    stored, _, slots_rows, width = memory_store.shape
    count, model = tokens.shape
    rows = query_weight.shape[0]

    cut = 2 * HEAD_SIZE
    late = width - cut
    early, joint = pl.pallas_call(
        functools.partial(join_kernel, cut),
        out_shape=(
            jax.ShapeDtypeStruct((rows, cut), jnp.bfloat16),
            jax.ShapeDtypeStruct((rows, late + width), jnp.bfloat16),
        ),
        name="join",
    )(query_weight, output_weight.T)
    joint = lax.all_gather(joint, "mem_0", axis=0, tiled=False)
    q_a = in_order(around(early, "mem_1", True), nx)
    q_a, joint = lax.optimization_barrier((q_a, joint))
    q_a = lax.all_gather(q_a, "mem_0", axis=0, tiled=False)

    owners = retrieved // stored
    offsets = retrieved % stored
    chosen = jnp.sum(jnp.where(owners == myself, offsets, 0), axis=1)
    picks = (chosen[:, None] * 2 + jnp.arange(per_frame, dtype=jnp.int32)[None]).reshape(-1)
    outgoing = jnp.take(memory_store.reshape(stored * 2, slots_rows, width), picks, axis=0)
    own_fresh = jnp.concatenate([fresh_entry[0], fresh_entry[1]], axis=1)
    extra = own_fresh.shape[1]
    own_fresh = jnp.pad(own_fresh, ((0, 0), (0, HEAD_SIZE - extra)))
    outgoing = jnp.concatenate(
        [outgoing, jnp.broadcast_to(own_fresh, (n_mem, *own_fresh.shape))], axis=2
    )
    incoming = lax.all_to_all(outgoing, MEM, split_axis=0, concat_axis=0, tiled=True)
    my_owners = lax.dynamic_index_in_dim(owners, myself // per_frame, 0, keepdims=False)
    fetched = jnp.take(incoming[:, :, :width], my_owners, axis=0).reshape(-1, width)
    other = lax.ppermute(fetched, "mem_1", [(i, i ^ 1) for i in range(nx)])
    even = myself % 2 == 0
    keys = jnp.where(even, fetched, other)
    vals = jnp.where(even, other, fetched)

    modrow = lax.dynamic_index_in_dim(time_modulation, timestep[0], 0, keepdims=False)
    values = tokens.astype(jnp.float32)
    factor = lax.rsqrt(jnp.mean(values * values, axis=1, keepdims=True) + EPS)
    modulated = (values * factor * (1.0 + modrow[0]) + modrow[1]).astype(jnp.bfloat16)

    joint, modulated, keys, vals = lax.optimization_barrier((joint, modulated, keys, vals))
    own = joint[:, :, :late]
    fore, back = shift(own, "mem_1", 1), shift(own, "mem_1", -1)
    low, high = shift(fore[: nz // 2], "mem_1", 1), shift(back[nz // 2:], "mem_1", -1)
    qb_all = ((own, 0, 0), (fore, -1, 0), (back, 1, 0), (low, 2, 0), (high, 2, nz // 2))

    fresh = incoming[:, :, width: width + extra].reshape(n_mem, slots_rows, 2, extra // 2)
    fresh = fresh.transpose(2, 1, 0, 3).reshape(2, slots_rows, width)
    slots = myself * stored + jnp.arange(stored, dtype=jnp.int32)
    updated_store = jnp.where(
        (slots == write_slot[0])[:, None, None, None], fresh[None], memory_store
    )

    ny, nc = lax.axis_size("tp_0"), lax.axis_size("tp_1")
    core = lax.axis_index("tp_1")
    swap = [(0, 1), (1, 0)]
    weight = joint[:, :, late:]
    away = lax.ppermute(weight, "tp_1", swap)
    weight = jnp.concatenate([weight, away], axis=2)
    weight = weight.reshape(ny, nc, rows, 2 * width)
    weight = lax.dynamic_slice_in_dim(
        jnp.concatenate([weight, weight], axis=0), lax.axis_index("tp_0"), ny, 0
    )
    weight = jnp.concatenate(
        [
            lax.dynamic_index_in_dim(weight, core, 1, keepdims=False),
            lax.dynamic_index_in_dim(weight, 1 - core, 1, keepdims=False),
        ],
        axis=1,
    )
    modulated, weight, updated_store = lax.optimization_barrier(
        (modulated, weight, updated_store)
    )

    pieces = [q_a]
    plan = [[((i, j), i, j, 0, cut) for i in range(nz) for j in range(nx)]]
    for array, off, low in qb_all:
        pieces.append(array)
        plan.append([(i, low + i, off, cut, late) for i in range(array.shape[0])])
    chunks = 4
    vmem = pl.BlockSpec(memory_space=pltpu.VMEM)
    hbm = pl.BlockSpec(memory_space=pltpu.HBM)
    half = jax.ShapeDtypeStruct((count // 2, width), jnp.bfloat16)
    keep, give = pl.pallas_call(
        functools.partial(attend_kernel, plan, rows, nx, chunks),
        out_shape=(half, half),
        in_specs=[hbm, vmem, vmem] + [hbm] * len(pieces),
        out_specs=(vmem, vmem),
        scratch_shapes=[
            pltpu.VMEM((count, model), jnp.bfloat16),
            pltpu.VMEM((model, width), jnp.bfloat16),
            pltpu.VMEM((count, width), jnp.float32),
            pltpu.VMEM((count, width), jnp.bfloat16),
            pltpu.SemaphoreType.DMA((chunks,)),
            pltpu.SemaphoreType.DMA((chunks,)),
        ],
        compiler_params=pltpu.CompilerParams(vmem_limit_bytes=62 * 1024 * 1024),
        cost_estimate=pl.CostEstimate(
            flops=2 * count * model * width, bytes_accessed=2 * model * width, transcendentals=0
        ),
        name="query_attend",
    )(modulated, keys, vals, *pieces)

    attended = jnp.concatenate([keep, lax.ppermute(give, "tp_1", swap)], axis=1)

    def term(d, group):
        return lax.dot_general(
            weight[d], group, (((1,), (1,)), ((), ())), preferred_element_type=jnp.float32
        ).astype(jnp.bfloat16)

    def terms(group):
        home = term(0, group)
        return [home] + [term(d, group) for d in range(1, ny)]

    def sent(parts):
        out = [parts[0]]
        for d in range(1, ny):
            out.append(shift(parts[d], "tp_0", d))
        return out

    def summed(parts):
        total = sum(part.astype(jnp.float32) for part in parts).astype(jnp.bfloat16)
        return total[:rows], total[rows:]

    def returned(block, by, mine):
        pairs = [
            (i * nc + c, (i + by) % nx * nc + (c if mine else 1 - c))
            for i in range(nx)
            for c in range(nc)
        ]
        return lax.ppermute(block, ("mem_1", "tp_1"), pairs)

    left, right = shift(attended, "mem_1", 1), shift(attended, "mem_1", -1)
    own_parts = sent(terms(attended))
    quarter = count // 4
    far = [shift(left[:quarter], "mem_1", 1), shift(right[quarter:], "mem_1", -1)]
    near_parts = sent(terms(jnp.concatenate([left, right], axis=0)))
    far_parts = sent(terms(jnp.concatenate(far, axis=0)))
    blocks, places = [], []
    groups = ((own_parts, (0,)), (near_parts, (-1, 1)), (far_parts, (2,)))
    for parts, bys in groups:
        both = summed(parts)
        for i, by in enumerate(bys):
            for mine in (1, 0):
                block = both[1 - mine][:, i * 2 * quarter: (i + 1) * 2 * quarter]
                blocks.append(block if mine and not by else returned(block, by, mine))
                places.append((-by, mine))
    memory_out = pl.pallas_call(
        functools.partial(place_kernel, places, nx),
        out_shape=jax.ShapeDtypeStruct((count, width), jnp.bfloat16),
        in_specs=[vmem] * len(blocks),
        out_specs=vmem,
        scratch_shapes=[pltpu.VMEM((width, count // 2), jnp.float32)],
        name="place",
    )(*blocks)

    return (memory_out, updated_store)


def solution(mesh):
    split = Mesh(mesh.devices.reshape(8, 4, 4, 2), MEM + TP)
    in_specs = (
        P(MEM, None),
        P(MEM, TP),
        P(TP, MEM),
        P(),
        P(),
        P(MEM, None, None, TP),
        P(),
        P(None, None, TP_MEM),
        P(),
    )
    out_specs = (P(MEM, TP), P(MEM, None, None, TP))
    return jax.shard_map(
        shards, mesh=split, in_specs=in_specs, out_specs=out_specs, check_vma=False
    )
```

```python
import functools

import jax
import jax.numpy as jnp
from jax import lax
from jax.experimental import pallas as pl
from jax.experimental.pallas import tpu as pltpu
from jax.sharding import Mesh
from jax.sharding import PartitionSpec as P

HEAD_SIZE = 128
MEM = ("mem_0", "mem_1")
TP = ("tp_0", "tp_1")
TP_MEM = TP + MEM

EPS = 1e-06


def shift(array, axis, by):
    n = lax.axis_size(axis)
    return lax.ppermute(array, axis, [(i, (i + by) % n) for i in range(n)])


def around(block, axis, whole, direction=1):
    n = lax.axis_size(axis)
    got = [(block, 0, None)]
    fore = back = block
    for step in range(1, (n - 1) // 2 + 1):
        fore, back = shift(fore, axis, 1), shift(back, axis, -1)
        got += [(fore, -step, None), (back, step, None)]
    half = n // 2
    if whole:
        last = shift(fore, axis, 1) if direction > 0 else shift(back, axis, -1)
        got.append((last, half, None))
    else:
        cut = block.shape[0] // 2
        got.append((shift(fore[:cut], axis, 1), half, (0, cut)))
        got.append((shift(back[cut:], axis, -1), half, (cut, block.shape[0])))
    return got


def in_order(got, n):
    return jnp.stack([next(a for a, off, _ in got if off % n == i) for i in range(n)])


def join_kernel(cut, q_ref, o_ref, joint_ref):
    joint_ref[:, : q_ref.shape[1] - cut] = q_ref[:, cut:]
    joint_ref[:, q_ref.shape[1] - cut:] = o_ref[...]


def attend_kernel(plan, rows, nx, chunks, xm_ref, k_ref, v_ref, *rest):
    pieces, rest = rest[: len(plan)], rest[len(plan):]
    keep_ref, give_ref, x_ref, w_ref, acc_ref, held_ref, x_sems, w_sems = rest
    x, core = lax.axis_index("mem_1"), lax.axis_index("tp_1")
    depth = w_ref.shape[0]
    step = depth // chunks
    entries = [
        (piece, *entry) for piece, part in zip(pieces, plan) for entry in part
    ]
    per_chunk = step // (rows * nx)
    for chunk in range(chunks):
        pltpu.make_async_copy(
            xm_ref.at[:, pl.ds(chunk * step, step)],
            x_ref.at[:, pl.ds(chunk * step, step)],
            x_sems.at[chunk],
        ).start()
        for piece, index, at_z, off_x, lane, lanes in entries:
            if at_z // per_chunk != chunk:
                continue
            block = at_z * nx + lax.rem(x + (off_x % nx), nx)
            start = pl.multiple_of(block * rows, 32)
            pltpu.make_async_copy(
                piece.at[index],
                w_ref.at[pl.ds(start, rows), pl.ds(lane, lanes)],
                w_sems.at[chunk],
            ).start()

    def accumulate(i, carry):
        at = pl.ds(pl.multiple_of(i * step, 128), step)
        pltpu.make_async_copy(x_ref.at[:, at], x_ref.at[:, at], x_sems.at[i]).wait()
        pltpu.make_async_copy(w_ref.at[at, :], w_ref.at[at, :], w_sems.at[i]).wait()
        acc_ref[...] += jnp.dot(x_ref[:, at], w_ref[at, :], preferred_element_type=jnp.float32)
        return carry

    acc_ref[...] = jnp.zeros_like(acc_ref)
    lax.fori_loop(0, chunks, accumulate, 0)
    half = acc_ref.shape[0] // 2

    def attend(i, carry):
        part = pl.ds(pl.multiple_of(i * half, half), half)
        for head in range(w_ref.shape[1] // HEAD_SIZE):
            at = pl.ds(head * HEAD_SIZE, HEAD_SIZE)
            query = acc_ref[part, at].astype(jnp.bfloat16)
            logits = lax.dot_general(
                query, k_ref[:, at], (((1,), (1,)), ((), ())), preferred_element_type=jnp.float32
            ) * HEAD_SIZE ** (-0.5)
            expo = jnp.exp(logits - jnp.max(logits, axis=-1, keepdims=True))
            probs = (expo / jnp.sum(expo, axis=-1, keepdims=True)).astype(jnp.bfloat16)
            held_ref[part, at] = jnp.dot(
                probs, v_ref[:, at], preferred_element_type=jnp.float32
            ).astype(jnp.bfloat16)
        return carry

    lax.fori_loop(0, 2, attend, 0)
    keep_ref[...] = held_ref[pl.ds(pl.multiple_of(core * half, half), half), :]
    give_ref[...] = held_ref[pl.ds(pl.multiple_of((1 - core) * half, half), half), :]


def place_kernel(offs, nx, *refs):
    pieces, (out_ref, held) = refs[: len(offs)], refs[len(offs):]
    x, core = lax.axis_index("mem_1"), lax.axis_index("tp_1")
    half = out_ref.shape[0] // 2
    for same in range(2):
        for piece, (off, mine) in zip(pieces, offs):
            if mine == same:
                rows = piece.shape[0]
                start = lax.rem(x + (off % nx), nx) * rows
                held[pl.ds(pl.multiple_of(start, 32), rows), :] = piece[...].astype(jnp.float32)
        to = core if same else 1 - core
        out_ref[pl.ds(pl.multiple_of(to * half, half), half), :] = held[...].T.astype(jnp.bfloat16)


def shards(
    tokens,
    query_weight,
    output_weight,
    time_modulation,
    timestep,
    memory_store,
    retrieved,
    fresh_entry,
    write_slot,
):
    nz, nx = lax.axis_size("mem_0"), lax.axis_size("mem_1")
    n_mem = nz * nx
    myself = lax.axis_index(MEM)
    frames = retrieved.shape[0]
    per_frame = n_mem // frames
    stored, _, slots_rows, width = memory_store.shape
    count, model = tokens.shape
    rows = query_weight.shape[0]

    cut = 2 * HEAD_SIZE
    late = width - cut
    joint = pl.pallas_call(
        functools.partial(join_kernel, cut),
        out_shape=jax.ShapeDtypeStruct((rows, late + width), jnp.bfloat16),
        name="join",
    )(query_weight, output_weight.T)
    query_weight, joint = lax.optimization_barrier((query_weight, joint))
    joint = lax.all_gather(joint, "mem_0", axis=0, tiled=False)
    q_a = in_order(around(query_weight[:, :cut], "mem_1", True), nx)
    q_a, joint = lax.optimization_barrier((q_a, joint))
    q_a = lax.all_gather(q_a, "mem_0", axis=0, tiled=False)

    owners = retrieved // stored
    offsets = retrieved % stored
    chosen = jnp.sum(jnp.where(owners == myself, offsets, 0), axis=1)
    picks = (chosen[:, None] * 2 + jnp.arange(per_frame, dtype=jnp.int32)[None]).reshape(-1)
    outgoing = jnp.take(memory_store.reshape(stored * 2, slots_rows, width), picks, axis=0)
    own_fresh = jnp.concatenate([fresh_entry[0], fresh_entry[1]], axis=1)
    extra = own_fresh.shape[1]
    own_fresh = jnp.pad(own_fresh, ((0, 0), (0, HEAD_SIZE - extra)))
    outgoing = jnp.concatenate(
        [outgoing, jnp.broadcast_to(own_fresh, (n_mem, *own_fresh.shape))], axis=2
    )
    incoming = lax.all_to_all(outgoing, MEM, split_axis=0, concat_axis=0, tiled=True)
    my_owners = lax.dynamic_index_in_dim(owners, myself // per_frame, 0, keepdims=False)
    fetched = jnp.take(incoming[:, :, :width], my_owners, axis=0).reshape(-1, width)
    other = lax.ppermute(fetched, "mem_1", [(i, i ^ 1) for i in range(nx)])
    even = myself % 2 == 0
    keys = jnp.where(even, fetched, other)
    vals = jnp.where(even, other, fetched)

    modrow = lax.dynamic_index_in_dim(time_modulation, timestep[0], 0, keepdims=False)
    values = tokens.astype(jnp.float32)
    factor = lax.rsqrt(jnp.mean(values * values, axis=1, keepdims=True) + EPS)
    modulated = (values * factor * (1.0 + modrow[0]) + modrow[1]).astype(jnp.bfloat16)

    joint, modulated, keys, vals = lax.optimization_barrier((joint, modulated, keys, vals))
    own = joint[:, :, :late]
    fore, back = shift(own, "mem_1", 1), shift(own, "mem_1", -1)
    low, high = shift(fore[: nz // 2], "mem_1", 1), shift(back[nz // 2:], "mem_1", -1)
    qb_all = ((own, 0, 0), (fore, -1, 0), (back, 1, 0), (low, 2, 0), (high, 2, nz // 2))

    fresh = incoming[:, :, width: width + extra].reshape(n_mem, slots_rows, 2, extra // 2)
    fresh = fresh.transpose(2, 1, 0, 3).reshape(2, slots_rows, width)
    slots = myself * stored + jnp.arange(stored, dtype=jnp.int32)
    updated_store = jnp.where(
        (slots == write_slot[0])[:, None, None, None], fresh[None], memory_store
    )

    ny, nc = lax.axis_size("tp_0"), lax.axis_size("tp_1")
    core = lax.axis_index("tp_1")
    swap = [(0, 1), (1, 0)]
    weight = joint[:, :, late:]
    away = lax.ppermute(weight, "tp_1", swap)
    weight = jnp.concatenate([weight, away], axis=2)
    weight = weight.reshape(ny, nc, rows, 2 * width)
    weight = lax.dynamic_slice_in_dim(
        jnp.concatenate([weight, weight], axis=0), lax.axis_index("tp_0"), ny, 0
    )
    weight = jnp.concatenate(
        [
            lax.dynamic_index_in_dim(weight, core, 1, keepdims=False),
            lax.dynamic_index_in_dim(weight, 1 - core, 1, keepdims=False),
        ],
        axis=1,
    )
    modulated, weight, updated_store = lax.optimization_barrier(
        (modulated, weight, updated_store)
    )

    pieces = [q_a]
    plan = [[((i, j), i, j, 0, cut) for i in range(nz) for j in range(nx)]]
    for array, off, low in qb_all:
        pieces.append(array)
        plan.append([(i, low + i, off, cut, late) for i in range(array.shape[0])])
    chunks = 4
    vmem = pl.BlockSpec(memory_space=pltpu.VMEM)
    hbm = pl.BlockSpec(memory_space=pltpu.HBM)
    half = jax.ShapeDtypeStruct((count // 2, width), jnp.bfloat16)
    keep, give = pl.pallas_call(
        functools.partial(attend_kernel, plan, rows, nx, chunks),
        out_shape=(half, half),
        in_specs=[hbm, vmem, vmem] + [hbm] * len(pieces),
        out_specs=(vmem, vmem),
        scratch_shapes=[
            pltpu.VMEM((count, model), jnp.bfloat16),
            pltpu.VMEM((model, width), jnp.bfloat16),
            pltpu.VMEM((count, width), jnp.float32),
            pltpu.VMEM((count, width), jnp.bfloat16),
            pltpu.SemaphoreType.DMA((chunks,)),
            pltpu.SemaphoreType.DMA((chunks,)),
        ],
        compiler_params=pltpu.CompilerParams(vmem_limit_bytes=62 * 1024 * 1024),
        cost_estimate=pl.CostEstimate(
            flops=2 * count * model * width, bytes_accessed=2 * model * width, transcendentals=0
        ),
        name="query_attend",
    )(modulated, keys, vals, *pieces)

    attended = jnp.concatenate([keep, lax.ppermute(give, "tp_1", swap)], axis=1)

    def term(d, group):
        return lax.dot_general(
            weight[d], group, (((1,), (1,)), ((), ())), preferred_element_type=jnp.float32
        ).astype(jnp.bfloat16)

    def terms(group):
        home = term(0, group)
        return [home] + [term(d, group) for d in range(1, ny)]

    def sent(parts):
        out = [parts[0]]
        for d in range(1, ny):
            out.append(shift(parts[d], "tp_0", d))
        return out

    def summed(parts):
        total = sum(part.astype(jnp.float32) for part in parts).astype(jnp.bfloat16)
        return total[:rows], total[rows:]

    def returned(block, by, mine):
        pairs = [
            (i * nc + c, (i + by) % nx * nc + (c if mine else 1 - c))
            for i in range(nx)
            for c in range(nc)
        ]
        return lax.ppermute(block, ("mem_1", "tp_1"), pairs)

    left, right = shift(attended, "mem_1", 1), shift(attended, "mem_1", -1)
    own_parts = sent(terms(attended))
    quarter = count // 4
    far = [shift(left[:quarter], "mem_1", 1), shift(right[quarter:], "mem_1", -1)]
    near_parts = sent(terms(jnp.concatenate([left, right], axis=0)))
    far_parts = sent(terms(jnp.concatenate(far, axis=0)))
    blocks, places = [], []
    groups = ((own_parts, (0,)), (near_parts, (-1, 1)), (far_parts, (2,)))
    for parts, bys in groups:
        both = summed(parts)
        for i, by in enumerate(bys):
            for mine in (1, 0):
                block = both[1 - mine][:, i * 2 * quarter: (i + 1) * 2 * quarter]
                blocks.append(block if mine and not by else returned(block, by, mine))
                places.append((-by, mine))
    memory_out = pl.pallas_call(
        functools.partial(place_kernel, places, nx),
        out_shape=jax.ShapeDtypeStruct((count, width), jnp.bfloat16),
        in_specs=[vmem] * len(blocks),
        out_specs=vmem,
        scratch_shapes=[pltpu.VMEM((width, count // 2), jnp.float32)],
        name="place",
    )(*blocks)

    return (memory_out, updated_store)


def solution(mesh):
    split = Mesh(mesh.devices.reshape(8, 4, 4, 2), MEM + TP)
    in_specs = (
        P(MEM, None),
        P(MEM, TP),
        P(TP, MEM),
        P(),
        P(),
        P(MEM, None, None, TP),
        P(),
        P(None, None, TP_MEM),
        P(),
    )
    out_specs = (P(MEM, TP), P(MEM, None, None, TP))
    return jax.shard_map(
        shards, mesh=split, in_specs=in_specs, out_specs=out_specs, check_vma=False
    )
```
